256 devices in a mesh: rep: 1, r: 32 (over y, z), s: 8 (over x, core).
Axes of the slice: x: 4, y: 4, z: 8, core: 2. Of those that a mesh axis runs over, the one named last changes fastest.
Arguments:
- x: bfloat16 [256, 2048, 512], P(('rep', 'r', 's'))
- dy: bfloat16 [256, 2048, 512], P(('rep', 'r', 's'))
- w_gate: bfloat16 [2, 512, 2048], P(None, 's')
- w_up: bfloat16 [2, 512, 2048], P(None, 's')
- w_down: bfloat16 [2, 2048, 512], P(None, 's')
- m_w_gate: float32 [2, 512, 2048], P(None, 's')
- m_w_up: float32 [2, 512, 2048], P(None, 's')
- m_w_down: float32 [2, 2048, 512], P(None, 's')
- v_w_gate: float32 [2, 512, 2048], P(None, 's')
- v_w_up: float32 [2, 512, 2048], P(None, 's')
- v_w_down: float32 [2, 2048, 512], P(None, 's')
Outputs:
- output 1: bfloat16 [2, 512, 2048], P('rep', 's')
- output 2: bfloat16 [2, 512, 2048], P('rep', 's')
- output 3: bfloat16 [2, 2048, 512], P('rep', 's')
- output 4: float32 [2, 512, 2048], P('rep', 's')
- output 5: float32 [2, 512, 2048], P('rep', 's')
- output 6: float32 [2, 2048, 512], P('rep', 's')
- output 7: float32 [2, 512, 2048], P('rep', 's')
- output 8: float32 [2, 512, 2048], P('rep', 's')
- output 9: float32 [2, 2048, 512], P('rep', 's')
All inputs are finite; a program needn't handle non-finite values.
Results may differ from the reference program's by a relative error of at most 0.022.
Values are sent between devices in bfloat16 or wider.
A program may use at most 768 MiB of HBM per device.

```python
import jax
import jax.numpy as jnp
from jax import lax

SEQUENCES = 256
TOKENS = 2048
D = 512
FF = 2048
LAYERS = 2
NAMES = ("w_gate", "w_up", "w_down")
SHAPES = {"w_gate": (LAYERS, D, FF), "w_up": (LAYERS, D, FF), "w_down": (LAYERS, FF, D)}


def bump(key, n, height):
    away = (jnp.arange(n, dtype=jnp.int32) - jax.random.randint(key, (), 0, n, jnp.int32)) % n
    return jnp.where(away < n // 8, height, 1.0)


def together(key, own, strength):
    shared = jax.random.normal(key, own.shape[1:], jnp.float32)
    return (own + strength * shared) * lax.rsqrt(1 + strength * strength)


def setup_inputs(seed: int = 0, part: int = 0) -> dict:
    kx, kdy, ka, kb, kz, kf, kh, kl, *keys = jax.random.split(jax.random.key(seed), 8 + 3 * len(NAMES))
    kx, kdy, ka, kb = (jax.random.fold_in(k, part) for k in (kx, kdy, ka, kb))
    kw, km, kv = (keys[i::3] for i in range(3))
    shape = (SEQUENCES, TOKENS, D)
    much_x, much_dy = jax.random.uniform(kz, (2,), jnp.float32, 0.0, 1.0)
    loud = 2.0 ** jax.random.uniform(jax.random.fold_in(kz, 1), (), jnp.float32, -1.0, 2.0)
    layers = 2.0 ** jax.random.uniform(kl, (LAYERS, 1, 1), jnp.float32, -1.0, 1.0)
    x = together(ka, jax.random.normal(kx, shape, jnp.float32), much_x) * bump(kf, D, 4.0)
    dy = together(kb, jax.random.normal(kdy, shape, jnp.float32), much_dy)
    drawn = {"x": x.astype(jnp.bfloat16), "dy": (loud * dy * (SEQUENCES * TOKENS) ** -0.5).astype(jnp.bfloat16)}
    for key, name in zip(kw, NAMES, strict=True):
        w = jax.random.normal(key, SHAPES[name], jnp.float32) * SHAPES[name][1] ** -0.5
        drawn[name] = (w * {"w_gate": 1.0, "w_up": bump(kh, FF, 4.0), "w_down": layers}[name]).astype(jnp.bfloat16)
    for key, name in zip(km, NAMES, strict=True):
        drawn[f"m_{name}"] = 0.1 * jax.random.normal(key, SHAPES[name], jnp.float32)
    for key, name in zip(kv, NAMES, strict=True):
        drawn[f"v_{name}"] = loud * loud * jax.random.uniform(key, SHAPES[name], jnp.float32, 0.05, 0.15)
    return drawn


def matmul(a, w):
    return jnp.dot(a, w, preferred_element_type=jnp.float32).astype(jnp.bfloat16)


def normed(h):
    wide = h.astype(jnp.float32)
    scale = lax.rsqrt(jnp.mean(wide**2, -1, keepdims=True) + 1e-6)
    return (wide * scale).astype(jnp.bfloat16)


def layer(h, w):
    a = normed(h)
    gate = jnp.dot(a, w["w_gate"], preferred_element_type=jnp.float32)
    up = jnp.dot(a, w["w_up"], preferred_element_type=jnp.float32)
    return h + matmul((jax.nn.silu(gate) * up).astype(jnp.bfloat16), w["w_down"])


def adamw(w, m, v, g):
    m = 0.9 * m + 0.1 * g
    v = 0.95 * v + 0.05 * g * g
    step = m * lax.rsqrt(v + 1e-8) + 0.1 * w
    return (w - 0.02 * step).astype(jnp.bfloat16), m, v


def stack(weights, h):
    return lax.scan(lambda h, w: (layer(h, w), None), h, weights)[0]


def reference(x, dy, w_gate, w_up, w_down, m_w_gate, m_w_up, m_w_down, v_w_gate, v_w_up, v_w_down):
    weights = dict(zip(NAMES, (w_gate, w_up, w_down), strict=True))

    def take(so_far, sequence):
        h, by_y = sequence
        _, back = jax.vjp(lambda w: stack(w, h), weights)
        return jax.tree.map(lambda total, term: total + term.astype(jnp.float32), so_far, back(by_y)[0]), None

    none_yet = {name: jnp.zeros(w.shape, jnp.float32) for name, w in weights.items()}
    by_weights, _ = lax.scan(take, none_yet, (x, dy))
    gradients = [by_weights[name].astype(jnp.bfloat16).astype(jnp.float32) for name in NAMES]
    new = [
        adamw(w.astype(jnp.float32), m, v, g)
        for w, m, v, g in zip((w_gate, w_up, w_down), (m_w_gate, m_w_up, m_w_down), (v_w_gate, v_w_up, v_w_down), gradients, strict=True)
    ]
    return tuple(one[which] for which in range(3) for one in new)
```

```python
import functools

import jax
import jax.numpy as jnp
from jax import lax
from jax.experimental import pallas as pl
from jax.experimental.pallas import tpu as pltpu
from jax.sharding import PartitionSpec as P

NAMES = ("w_gate", "w_up", "w_down")
MESH = pl.DeviceIdType.MESH
RING = 4
HALVES = 2


def matmul(a, w):
    return jnp.dot(a, w, preferred_element_type=jnp.float32).astype(jnp.bfloat16)


def normed(h):
    wide = h.astype(jnp.float32)
    scale = lax.rsqrt(jnp.mean(wide**2, -1, keepdims=True) + 1e-6)
    return (wide * scale).astype(jnp.bfloat16)


def layer(h, w):
    a = normed(h)
    gate = jnp.dot(a, w["w_gate"], preferred_element_type=jnp.float32)
    up = jnp.dot(a, w["w_up"], preferred_element_type=jnp.float32)
    return h + matmul((jax.nn.silu(gate) * up).astype(jnp.bfloat16), w["w_down"])


def adamw(w, m, v, g):
    m = 0.9 * m + 0.1 * g
    v = 0.95 * v + 0.05 * g * g
    step = m * lax.rsqrt(v + 1e-8) + 0.1 * w
    return (w - 0.02 * step).astype(jnp.bfloat16), m, v


class Place:
    def __init__(self, nz):
        self.nz = nz
        r, s = lax.axis_index("r"), lax.axis_index("s")
        self.y, self.z, self.x, self.core, self.s, self.r = r // nz, r % nz, s // 2, s % 2, s, r
        self.partner = {"s": 2 * self.x + 1 - self.core}

    def at_x(self, d):
        return (self.x + d) % RING

    def at_y(self, d):
        return (self.y + d) % RING

    def at_z(self, d):
        return (self.z + d) % self.nz

    def to_x(self, d):
        return {"s": 2 * self.at_x(d) + self.core}

    def to_y(self, d):
        return {"r": self.at_y(d) * self.nz + self.z}

    def to_z(self, d):
        return {"r": self.y * self.nz + self.at_z(d)}


def meet(peers):
    barrier = pltpu.get_barrier_semaphore()
    for peer in peers:
        pl.semaphore_signal(barrier, inc=1, device_id=peer, device_id_type=MESH)
    pl.semaphore_wait(barrier, len(peers))


def send(src, dst, sems, device):
    send_sem, recv_sem = sems
    return pltpu.make_async_remote_copy(
        src_ref=src, dst_ref=dst, send_sem=send_sem, recv_sem=recv_sem, device_id=device, device_id_type=MESH
    )


def gather_kernel(nz, layers, *refs):
    ins, outs, (snd, rcv, loc) = refs[:3], refs[3:6], refs[6:]
    p = Place(nz)
    meet([p.partner, p.to_x(1), p.to_x(-1)])

    def block(i, l, x, core, half=None):
        ref = outs[i].at[l, 2 * x + core]
        if half is None:
            return ref
        rows = ref.shape[0] // 2
        return ref.at[pl.ds(half * rows, rows)]

    def copy(k, i, l, what):
        n = 3 * l + i
        sems = (snd.at[n, k], rcv.at[n, k])
        (src_x, half), device = what
        b = block(i, l, src_x, p.core, half)
        return send(b, b, sems, device)

    def own(i, l):
        return ins[i].at[l]

    todo = [(i, l) for l in range(layers) for i in range(3)]
    for i, l in todo:
        n = 3 * l + i
        mine = block(i, l, p.x, p.core)
        pltpu.make_async_copy(own(i, l), mine, loc.at[n]).start()
        for k, device in ((0, p.to_x(1)), (1, p.to_x(-1)), (2, p.partner)):
            send(own(i, l), mine, (snd.at[n, k], rcv.at[n, k]), device).start()
    started = []
    for i, l in todo:
        n = 3 * l + i
        for k in (0, 1):
            send(own(i, l), block(i, l, p.x, p.core), (snd.at[n, k], rcv.at[n, k]), p.to_x(1)).wait_recv()
            src = p.at_x(-1 if k == 0 else 1)
            on = copy(3 + k, i, l, ((src, k), p.to_x(1 if k == 0 else -1)))
            on.start()
            over = copy(5 + k, i, l, ((src, None), p.partner))
            over.start()
            started += [on, over]
    for i, l in todo:
        for k in (0, 1):
            copy(3 + k, i, l, ((p.at_x(2), k), p.to_x(1))).wait_recv()
            over = copy(7 + k, i, l, ((p.at_x(2), k), p.partner))
            over.start()
            started += [over]
    for i, l in todo:
        n = 3 * l + i
        send(own(i, l), block(i, l, p.x, p.core), (snd.at[n, 2], rcv.at[n, 2]), p.partner).wait_recv()
        for k in (5, 6):
            copy(k, i, l, ((p.x, None), p.partner)).wait_recv()
        for k in (7, 8):
            copy(k, i, l, ((p.x, k - 7), p.partner)).wait_recv()
        pltpu.make_async_copy(own(i, l), block(i, l, p.x, p.core), loc.at[n]).wait()
        for k in (0, 1, 2):
            send(own(i, l), block(i, l, p.x, p.core), (snd.at[n, k], rcv.at[n, k]), p.partner).wait_send()
    for one in started:
        one.wait_send()


def gather(mesh, weights):
    layers = weights[0].shape[0]
    nz = mesh.shape["r"] // RING
    n = 3 * layers
    return pl.pallas_call(
        functools.partial(gather_kernel, nz, layers),
        out_shape=[jax.ShapeDtypeStruct((layers, 2 * RING) + w.shape[1:], w.dtype) for w in weights],
        in_specs=[pl.BlockSpec(memory_space=pl.ANY)] * 3,
        out_specs=[pl.BlockSpec(memory_space=pltpu.VMEM)] * 3,
        scratch_shapes=[
            pltpu.SemaphoreType.DMA((n, 9)),
            pltpu.SemaphoreType.DMA((n, 9)),
            pltpu.SemaphoreType.DMA((n,)),
        ],
        compiler_params=pltpu.CompilerParams(collective_id=0, has_side_effects=True, vmem_limit_bytes=48 * 2**20),
        name="gather",
    )(*weights)


def pieces(rows, columns, by_rows):
    qr, qc = (rows // RING, columns) if by_rows else (rows, columns // RING)
    across = qc // 128
    return [
        [
            (slice((q * qr if by_rows else 0) + 16 * (k // across), (q * qr if by_rows else 0) + 16 * (k // across) + 16),
             slice((0 if by_rows else q * qc) + 128 * (k % across), (0 if by_rows else q * qc) + 128 * (k % across) + 128))
            for k in range(qr // 16 * across)
        ]
        for q in range(RING)
    ]


def wide(ref):
    return ref.astype(jnp.float32)


SCRATCH = ("dg", "dd", "part", "x1", "x2", "yb", "y1", "y2", "zb", "zr", "out", "sem_d", "sem_l", "sem_z")


def reduce_scratch(nz, chunks, gate_block, down_block):
    bf = functools.partial(pltpu.VMEM, dtype=jnp.bfloat16)
    piece = (48, 128)
    return [
        pltpu.VMEM((chunks, 2, RING) + gate_block, jnp.bfloat16),
        pltpu.VMEM((chunks, RING) + down_block, jnp.bfloat16),
        pltpu.VMEM((chunks, RING, RING, nz) + piece, jnp.bfloat16),
        pltpu.VMEM((chunks, 2, RING // 2, nz) + piece, jnp.bfloat16),
        pltpu.VMEM((chunks, 2, RING, nz) + piece, jnp.bfloat16),
        pltpu.VMEM((chunks, RING, nz) + piece, jnp.bfloat16),
        pltpu.VMEM((chunks, 2, nz // 2) + piece, jnp.bfloat16),
        pltpu.VMEM((chunks, 2, nz) + piece, jnp.bfloat16),
        pltpu.VMEM((chunks, nz) + piece, jnp.bfloat16),
        pltpu.VMEM((chunks, nz) + piece, jnp.bfloat16),
        pltpu.VMEM((chunks, RING, nz) + piece, jnp.bfloat16),
        pltpu.SemaphoreType.DMA((2, chunks, 3)),
        pltpu.SemaphoreType.DMA((2, chunks, 6, 2)),
        pltpu.SemaphoreType.DMA((2, chunks, 2, nz)),
    ]


class Reduce:
    def __init__(self, p, bufs, own, gate_block, down_block, finish):
        self.p, self.own, self.finish = p, own, finish
        for name, ref in zip(SCRATCH, bufs, strict=True):
            setattr(self, name, ref)
        self.gate, self.down = pieces(*gate_block, False), pieces(*down_block, True)
        self.stages = [self.s0, self.s1, self.s2, self.s3, self.s4, self.s5, self.s6, self.s7, self.s8, self.s9]

    def peers(self):
        p = self.p
        return [p.partner, p.to_x(1), p.to_x(-1), p.to_y(1), p.to_y(-1)] + [p.to_z(d) for d in range(1, p.nz)]

    def link(self, h, k, way, src, dst, device):
        return send(src, dst, (self.sem_l.at[0, h, k, way], self.sem_l.at[1, h, k, way]), device)

    def d2d(self, h, core):
        own = self.own(h)
        dst = [self.dg.at[h, 0], self.dg.at[h, 1], self.dd.at[h]]
        return [
            send(own[i](core), dst[i], (self.sem_d.at[0, h, i], self.sem_d.at[1, h, i]), self.p.partner) for i in range(3)
        ]

    def s0(self, h):
        for one in self.d2d(h, 1 - self.p.core):
            one.start()

    def xs1(self, h):
        p = self.p
        block = self.part.at[h, p.at_x(2)]
        return [
            self.link(h, 0, 0, block.at[pl.ds(0, 2)], self.x1.at[h, 0], p.to_x(1)),
            self.link(h, 0, 1, block.at[pl.ds(2, 2)], self.x1.at[h, 1], p.to_x(-1)),
        ]

    def xs2(self, h):
        p = self.p
        return [
            self.link(h, 1, 0, self.part.at[h, p.at_x(1)], self.x2.at[h, 0], p.to_x(1)),
            self.link(h, 1, 1, self.part.at[h, p.at_x(-1)], self.x2.at[h, 1], p.to_x(-1)),
        ]

    def ys1(self, h):
        p = self.p
        block, half = self.yb.at[h, p.at_y(2)], p.nz // 2
        return [
            self.link(h, 2, 0, block.at[pl.ds(0, half)], self.y1.at[h, 0], p.to_y(1)),
            self.link(h, 2, 1, block.at[pl.ds(half, half)], self.y1.at[h, 1], p.to_y(-1)),
        ]

    def ys2(self, h):
        p = self.p
        return [
            self.link(h, 3, 0, self.yb.at[h, p.at_y(1)], self.y2.at[h, 0], p.to_y(1)),
            self.link(h, 3, 1, self.yb.at[h, p.at_y(-1)], self.y2.at[h, 1], p.to_y(-1)),
        ]

    def zs(self, h, d):
        p = self.p
        to = p.at_z(d)
        return send(self.zb.at[h, to], self.zr.at[h, p.z], (self.sem_z.at[0, h, 0, to], self.sem_z.at[1, h, 0, p.z]), p.to_z(d))

    def zs_from(self, h, d):
        p = self.p
        src = p.at_z(d)
        return send(self.zb.at[h, src], self.zr.at[h, src], (self.sem_z.at[0, h, 0, src], self.sem_z.at[1, h, 0, src]), p.to_z(d))

    def za(self, h, d):
        p = self.p
        mine = self.out.at[h, p.y, p.z]
        return send(mine, mine, (self.sem_z.at[0, h, 1, p.at_z(d)], self.sem_z.at[1, h, 1, p.z]), p.to_z(d))

    def za_from(self, h, d):
        p = self.p
        src = p.at_z(d)
        piece = self.out.at[h, p.y, src]
        return send(piece, piece, (self.sem_z.at[0, h, 1, src], self.sem_z.at[1, h, 1, src]), p.to_z(d))

    def ya1(self, h, y=None):
        p = self.p
        piece = self.out.at[h, p.y]
        return [self.link(h, 4, 0, piece, piece, p.to_y(1)), self.link(h, 4, 1, piece, piece, p.to_y(-1))]

    def ya1_from(self, h):
        p = self.p
        below, above = self.out.at[h, p.at_y(-1)], self.out.at[h, p.at_y(1)]
        return [self.link(h, 4, 0, below, below, p.to_y(1)), self.link(h, 4, 1, above, above, p.to_y(-1))]

    def ya2(self, h, first, second):
        p, half = self.p, self.p.nz // 2
        a, b = self.out.at[h, first, pl.ds(0, half)], self.out.at[h, second, pl.ds(half, half)]
        return [self.link(h, 5, 0, a, a, p.to_y(1)), self.link(h, 5, 1, b, b, p.to_y(-1))]

    def s1(self, h):
        p = self.p
        for one in self.d2d(h, 1 - p.core):
            one.wait_recv()
        own = self.own(h)

        def block(x, _):
            for i, cut in ((0, self.gate), (1, self.gate), (2, self.down)):
                mine = own[i](p.core).at[x]
                theirs = self.dd.at[h, x] if i == 2 else self.dg.at[h, i, x]
                for q in range(RING):
                    for k, (rows, columns) in enumerate(cut[q]):
                        total = wide(mine[rows, columns]) + wide(theirs[rows, columns])
                        self.part[h, x, q, k, 16 * i : 16 * i + 16, :] = total.astype(jnp.bfloat16)
            return 0

        lax.fori_loop(0, RING, block, 0)
        for one in self.xs1(h):
            one.start()

    def s2(self, h):
        p = self.p
        for way, one in enumerate(self.xs1(h)):
            one.wait_recv()
        for way in (0, 1):
            to = p.at_x(1 if way == 0 else -1)

            def add(k, _):
                q, kk = 2 * way + k // p.nz, k % p.nz
                total = wide(self.part[h, to, q, kk]) + wide(self.x1[h, way, k // p.nz, kk])
                self.part[h, to, q, kk] = total.astype(jnp.bfloat16)
                return 0

            lax.fori_loop(0, 2 * p.nz, add, 0)
            self.xs2(h)[way].start()

    def s3(self, h):
        p = self.p
        for one in self.xs2(h):
            one.wait_recv()

        def add(k, _):
            q, kk = k // p.nz, k % p.nz
            total = wide(self.part[h, p.x, q, kk]) + (wide(self.x2[h, 0, q, kk]) + wide(self.x2[h, 1, q, kk]))
            self.yb[h, q, kk] = total.astype(jnp.bfloat16)
            return 0

        lax.fori_loop(0, RING * p.nz, add, 0)
        for one in self.ys1(h):
            one.start()

    def s4(self, h):
        p, half = self.p, self.p.nz // 2
        for one in self.ys1(h):
            one.wait_recv()
        for way in (0, 1):
            to = p.at_y(1 if way == 0 else -1)
            for k in range(half):
                kk = way * half + k
                self.yb[h, to, kk] = (wide(self.yb[h, to, kk]) + wide(self.y1[h, way, k])).astype(jnp.bfloat16)
            self.ys2(h)[way].start()

    def s5(self, h):
        p = self.p
        for one in self.ys2(h):
            one.wait_recv()
        for k in range(p.nz):
            total = wide(self.yb[h, p.y, k]) + (wide(self.y2[h, 0, k]) + wide(self.y2[h, 1, k]))
            self.zb[h, k] = total.astype(jnp.bfloat16)
        for d in range(1, p.nz):
            self.zs(h, d).start()

    def s6(self, h):
        p = self.p
        total = wide(self.zb[h, p.z])
        for d in range(1, p.nz):
            self.zs_from(h, d).wait_recv()
            total += wide(self.zr[h, p.at_z(d)])
        self.out[h, p.y, p.z] = total.astype(jnp.bfloat16)
        for d in range(1, p.nz):
            self.za(h, d).start()

    def s7(self, h):
        for d in range(1, self.p.nz):
            self.za_from(h, d).wait_recv()
        for one in self.ya1(h):
            one.start()

    def s8(self, h):
        p = self.p
        for one in self.ya1_from(h):
            one.wait_recv()
        for one in self.ya2(h, p.at_y(-1), p.at_y(1)):
            one.start()

    def s9(self, h):
        p = self.p
        for one in self.ya2(h, p.at_y(2), p.at_y(2)):
            one.wait_recv()
        self.finish(h)

    def drain(self, h):
        p = self.p
        for one in self.d2d(h, 1 - p.core) + self.xs1(h) + self.xs2(h) + self.ys1(h) + self.ys2(h):
            one.wait_send()
        for d in range(1, p.nz):
            self.zs(h, d).wait_send()
            self.za(h, d).wait_send()
        for one in self.ya1(h) + self.ya2(h, p.at_y(-1), p.at_y(1)):
            one.wait_send()

    def unpack(self, h, i, dst):
        for q in range(RING):
            for k, (rows, columns) in enumerate((self.down if i == 2 else self.gate)[q]):
                dst[rows, columns] = self.out[h, q, k, 16 * i : 16 * i + 16, :]


def reduce_kernel(nz, chunks, gate_block, down_block, *refs):
    ins, outs, bufs = refs[:3], refs[3:6], refs[6:]
    p = Place(nz)

    def own(h):
        l, b = chunks // HALVES - 1 - h // HALVES, h % HALVES

        def gate(ref):
            return lambda core: ref.at[l, :, core, :, pl.ds(pl.multiple_of(b * gate_block[1], 128), gate_block[1])]

        def down(core):
            return ins[2].at[l, :, core, pl.ds(pl.multiple_of(b * down_block[0], 16), down_block[0])]

        return gate(ins[0]), gate(ins[1]), down

    def finish(h):
        l, b = chunks // HALVES - 1 - h // HALVES, h % HALVES
        for i in (0, 1):
            red.unpack(h, i, outs[i].at[l, :, pl.ds(pl.multiple_of(b * gate_block[1], 128), gate_block[1])])
        red.unpack(h, 2, outs[2].at[l, pl.ds(pl.multiple_of(b * down_block[0], 16), down_block[0])])

    red = Reduce(p, bufs, own, gate_block, down_block, finish)
    meet(red.peers())

    def tick(t, _):
        for k, stage in enumerate(red.stages):
            h = t - k

            @pl.when((h >= 0) & (h < chunks))
            def _():
                stage(h)

        return 0

    lax.fori_loop(0, chunks + len(red.stages) - 1, tick, 0)

    def drain(h, _):
        red.drain(h)
        return 0

    lax.fori_loop(0, chunks, drain, 0)


def reduce(mesh, terms):
    nz = mesh.shape["r"] // RING
    layers = terms[0].shape[0]
    chunks = layers * HALVES
    rows, columns = terms[0].shape[3:]
    gate_block = (rows, columns // HALVES)
    rows, columns = terms[2].shape[3:]
    down_block = (rows // HALVES, columns)
    return pl.pallas_call(
        functools.partial(reduce_kernel, nz, chunks, gate_block, down_block),
        out_shape=[jax.ShapeDtypeStruct((layers,) + t.shape[3:], t.dtype) for t in terms],
        in_specs=[pl.BlockSpec(memory_space=pltpu.VMEM)] * 3,
        out_specs=[pl.BlockSpec(memory_space=pltpu.VMEM)] * 3,
        scratch_shapes=reduce_scratch(nz, chunks, gate_block, down_block),
        compiler_params=pltpu.CompilerParams(collective_id=1, has_side_effects=True, vmem_limit_bytes=60 * 2**20),
        name="reduce",
    )(*terms)


def solution(mesh):
    def step(x, dy, *arrays):
        weights, m, v = (arrays[i : i + 3] for i in (0, 3, 6))
        layers = weights[0].shape[0]
        whole = gather(mesh, weights)
        fetched = [
            {name: w[l].reshape(-1, w.shape[-1]) for name, w in zip(NAMES, whole, strict=True)} for l in range(layers)
        ]
        h, kept = x[0], []
        for number in range(layers):
            kept.append(h)
            h = layer(h, fetched[number])
        by_h, terms = dy[0], [None] * layers
        for number in reversed(range(layers)):
            _, back = jax.vjp(lambda w, h: layer(h, w), fetched[number], kept[number])
            by_w, by_h = back(by_h)
            terms[number] = by_w
        stacked = [
            jnp.stack([terms[l][name] for l in range(layers)]).reshape(layers, RING, 2, *w.shape[1:])
            for name, w in zip(NAMES, weights, strict=True)
        ]
        gradients = [g.astype(jnp.float32) for g in reduce(mesh, stacked)]
        new = [adamw(w.astype(jnp.float32), m, v, g) for w, m, v, g in zip(weights, m, v, gradients, strict=True)]
        return tuple(one[which] for which in range(3) for one in new)

    states, cut = P(("rep", "r", "s"), None, None), P(None, "s", None)
    return jax.shard_map(
        step,
        mesh=mesh,
        in_specs=(states, states) + (cut,) * 9,
        out_specs=(P("rep", "s", None),) * 9,
        check_vma=False,
    )
```

```python
import functools

import jax
import jax.numpy as jnp
from jax import lax
from jax.experimental import pallas as pl
from jax.experimental.pallas import tpu as pltpu
from jax.sharding import PartitionSpec as P

NAMES = ("w_gate", "w_up", "w_down")
MESH = pl.DeviceIdType.MESH
RING = 4


def adamw(w, m, v, g):
    m = 0.9 * m + 0.1 * g
    v = 0.95 * v + 0.05 * g * g
    step = m * lax.rsqrt(v + 1e-8) + 0.1 * w
    return (w - 0.02 * step).astype(jnp.bfloat16), m, v


class Place:
    def __init__(self, nz):
        self.nz = nz
        r, s = lax.axis_index("r"), lax.axis_index("s")
        self.y, self.z, self.x, self.core, self.s, self.r = r // nz, r % nz, s // 2, s % 2, s, r
        self.partner = {"s": 2 * self.x + 1 - self.core}

    def at_x(self, d):
        return (self.x + d) % RING

    def at_y(self, d):
        return (self.y + d) % RING

    def at_z(self, d):
        return (self.z + d) % self.nz

    def to_x(self, d):
        return {"s": 2 * self.at_x(d) + self.core}

    def to_y(self, d):
        return {"r": self.at_y(d) * self.nz + self.z}

    def to_z(self, d):
        return {"r": self.y * self.nz + self.at_z(d)}


def meet(peers):
    barrier = pltpu.get_barrier_semaphore()
    for peer in peers:
        pl.semaphore_signal(barrier, inc=1, device_id=peer, device_id_type=MESH)
    pl.semaphore_wait(barrier, len(peers))


def send(src, dst, sems, device):
    send_sem, recv_sem = sems
    return pltpu.make_async_remote_copy(
        src_ref=src, dst_ref=dst, send_sem=send_sem, recv_sem=recv_sem, device_id=device, device_id_type=MESH
    )


class Gather:
    def __init__(self, p, ins, outs, snd, rcv, loc):
        self.p, self.ins, self.outs, self.snd, self.rcv, self.loc = p, ins, outs, snd, rcv, loc

    def block(self, l, i, x, half=None):
        ref = self.outs[i].at[l, 2 * x + self.p.core]
        if half is None:
            return ref
        rows = ref.shape[0] // 2
        return ref.at[pl.ds(half * rows, rows)]

    def copy(self, l, i, k, src, dst, device):
        return send(src, dst, (self.snd.at[3 * l + i, k], self.rcv.at[3 * l + i, k]), device)

    def own(self, l, i, k):
        p = self.p
        return self.copy(l, i, k, self.ins[i].at[l], self.block(l, i, p.x), (p.to_x(1), p.to_x(-1), p.partner)[k])

    def local(self, l, i):
        return pltpu.make_async_copy(self.ins[i].at[l], self.block(l, i, self.p.x), self.loc.at[3 * l + i])

    def on(self, l, i, k):
        p = self.p
        b = self.block(l, i, p.at_x(-1 if k == 0 else 1), k)
        return self.copy(l, i, 3 + k, b, b, p.to_x(1 if k == 0 else -1))

    def over(self, l, i, k):
        p = self.p
        b = self.block(l, i, p.at_x((-1, 1, 2, 2)[k]), (None, None, 0, 1)[k])
        return self.copy(l, i, 5 + k, b, b, p.partner)

    def first(self, l, i):
        self.local(l, i).start()
        for k in range(3):
            self.own(l, i, k).start()

    def second(self, l, i):
        for k in (0, 1):
            self.own(l, i, k).wait_recv()
            self.on(l, i, k).start()
            self.over(l, i, k).start()

    def third(self, l, i):
        for k in (0, 1):
            self.on(l, i, k).wait_recv()
            self.over(l, i, 2 + k).start()

    def last(self, l, i):
        self.own(l, i, 2).wait_recv()
        for k in range(4):
            self.over(l, i, k).wait_recv()
        self.local(l, i).wait()

    def drain(self, l, i):
        for k in range(3):
            self.own(l, i, k).wait_send()
        for k in (0, 1):
            self.on(l, i, k).wait_send()
        for k in range(4):
            self.over(l, i, k).wait_send()


def pieces(rows, columns, by_rows):
    qr, qc = (rows // RING, columns) if by_rows else (rows, columns // RING)
    across = qc // 128
    return [
        [
            (slice((q * qr if by_rows else 0) + 16 * (k // across), (q * qr if by_rows else 0) + 16 * (k // across) + 16),
             slice((0 if by_rows else q * qc) + 128 * (k % across), (0 if by_rows else q * qc) + 128 * (k % across) + 128))
            for k in range(qr // 16 * across)
        ]
        for q in range(RING)
    ]


def wide(ref):
    return ref.astype(jnp.float32)


SCRATCH = ("dg", "dd", "part", "x1", "x2", "yb", "y1", "y2", "zb", "zr", "out", "sem_d", "sem_l", "sem_z")


def reduce_scratch(nz, chunks, gate_block, down_block):
    bf = functools.partial(pltpu.VMEM, dtype=jnp.bfloat16)
    piece = (48, 128)
    return [
        pltpu.VMEM((2, 2, RING) + gate_block, jnp.bfloat16),
        pltpu.VMEM((2, RING) + down_block, jnp.bfloat16),
        pltpu.VMEM((chunks, RING, RING, nz) + piece, jnp.bfloat16),
        pltpu.VMEM((chunks, 2, RING // 2, nz) + piece, jnp.bfloat16),
        pltpu.VMEM((chunks, 2, RING, nz) + piece, jnp.bfloat16),
        pltpu.VMEM((chunks, RING, nz) + piece, jnp.bfloat16),
        pltpu.VMEM((chunks, 2, nz // 2) + piece, jnp.bfloat16),
        pltpu.VMEM((chunks, 2, nz) + piece, jnp.bfloat16),
        pltpu.VMEM((chunks, nz) + piece, jnp.bfloat16),
        pltpu.VMEM((chunks, nz) + piece, jnp.bfloat16),
        pltpu.VMEM((chunks, RING, nz) + piece, jnp.bfloat16),
        pltpu.SemaphoreType.DMA((2, chunks, 3)),
        pltpu.SemaphoreType.DMA((2, chunks, 6, 2)),
        pltpu.SemaphoreType.DMA((2, chunks, 2, nz)),
    ]


class Reduce:
    def __init__(self, p, bufs, own, gate_block, down_block, finish):
        self.p, self.own, self.finish = p, own, finish
        for name, ref in zip(SCRATCH, bufs, strict=True):
            setattr(self, name, ref)
        self.down_rows = down_block[0]
        self.gate, self.down = pieces(*gate_block, False), pieces(*down_block, True)
        self.stages = [self.s0, self.s1, self.s2, self.s3, self.s4, self.s5, self.s6, self.s7, self.s8, self.s9]

    def peers(self):
        p = self.p
        return [p.partner, p.to_x(1), p.to_x(-1), p.to_y(1), p.to_y(-1)] + [p.to_z(d) for d in range(1, p.nz)]

    def link(self, h, k, way, src, dst, device):
        return send(src, dst, (self.sem_l.at[0, h, k, way], self.sem_l.at[1, h, k, way]), device)

    def d2d(self, h, core):
        own = self.own(h)
        dst = [self.dg.at[h % 2, 0], self.dg.at[h % 2, 1], self.dd.at[h % 2]]
        return [
            send(own[i](core), dst[i], (self.sem_d.at[0, h, i], self.sem_d.at[1, h, i]), self.p.partner) for i in range(3)
        ]

    def s0(self, h):
        for one in self.d2d(h, 1 - self.p.core):
            one.start()

    def xs1(self, h):
        p = self.p
        block = self.part.at[h, p.at_x(2)]
        return [
            self.link(h, 0, 0, block.at[pl.ds(0, 2)], self.x1.at[h, 0], p.to_x(1)),
            self.link(h, 0, 1, block.at[pl.ds(2, 2)], self.x1.at[h, 1], p.to_x(-1)),
        ]

    def xs2(self, h):
        p = self.p
        return [
            self.link(h, 1, 0, self.part.at[h, p.at_x(1)], self.x2.at[h, 0], p.to_x(1)),
            self.link(h, 1, 1, self.part.at[h, p.at_x(-1)], self.x2.at[h, 1], p.to_x(-1)),
        ]

    def ys1(self, h):
        p = self.p
        block, half = self.yb.at[h, p.at_y(2)], p.nz // 2
        return [
            self.link(h, 2, 0, block.at[pl.ds(0, half)], self.y1.at[h, 0], p.to_y(1)),
            self.link(h, 2, 1, block.at[pl.ds(half, half)], self.y1.at[h, 1], p.to_y(-1)),
        ]

    def ys2(self, h):
        p = self.p
        return [
            self.link(h, 3, 0, self.yb.at[h, p.at_y(1)], self.y2.at[h, 0], p.to_y(1)),
            self.link(h, 3, 1, self.yb.at[h, p.at_y(-1)], self.y2.at[h, 1], p.to_y(-1)),
        ]

    def zs(self, h, d):
        p = self.p
        to = p.at_z(d)
        return send(self.zb.at[h, to], self.zr.at[h, p.z], (self.sem_z.at[0, h, 0, to], self.sem_z.at[1, h, 0, p.z]), p.to_z(d))

    def zs_from(self, h, d):
        p = self.p
        src = p.at_z(d)
        return send(self.zb.at[h, src], self.zr.at[h, src], (self.sem_z.at[0, h, 0, src], self.sem_z.at[1, h, 0, src]), p.to_z(d))

    def za(self, h, d):
        p = self.p
        mine = self.out.at[h, p.y, p.z]
        return send(mine, mine, (self.sem_z.at[0, h, 1, p.at_z(d)], self.sem_z.at[1, h, 1, p.z]), p.to_z(d))

    def za_from(self, h, d):
        p = self.p
        src = p.at_z(d)
        piece = self.out.at[h, p.y, src]
        return send(piece, piece, (self.sem_z.at[0, h, 1, src], self.sem_z.at[1, h, 1, src]), p.to_z(d))

    def ya1(self, h, y=None):
        p = self.p
        piece = self.out.at[h, p.y]
        return [self.link(h, 4, 0, piece, piece, p.to_y(1)), self.link(h, 4, 1, piece, piece, p.to_y(-1))]

    def ya1_from(self, h):
        p = self.p
        below, above = self.out.at[h, p.at_y(-1)], self.out.at[h, p.at_y(1)]
        return [self.link(h, 4, 0, below, below, p.to_y(1)), self.link(h, 4, 1, above, above, p.to_y(-1))]

    def ya2(self, h, first, second):
        p, half = self.p, self.p.nz // 2
        a, b = self.out.at[h, first, pl.ds(0, half)], self.out.at[h, second, pl.ds(half, half)]
        return [self.link(h, 5, 0, a, a, p.to_y(1)), self.link(h, 5, 1, b, b, p.to_y(-1))]

    def s1(self, h):
        p = self.p
        for one in self.d2d(h, 1 - p.core):
            one.wait_recv()
            one.wait_send()
        own = self.own(h)

        def block(x, _):
            for i, cut in ((0, self.gate), (1, self.gate), (2, self.down)):
                mine = own[i](p.core).at[x]
                theirs = self.dd.at[h % 2, x] if i == 2 else self.dg.at[h % 2, i, x]
                for q in range(RING):
                    for k, (rows, columns) in enumerate(cut[q]):
                        total = wide(mine[rows, columns]) + wide(theirs[rows, columns])
                        self.part[h, x, q, k, 16 * i : 16 * i + 16, :] = total.astype(jnp.bfloat16)
            return 0

        lax.fori_loop(0, RING, block, 0)
        for one in self.xs1(h):
            one.start()

    def s2(self, h):
        p = self.p
        for way, one in enumerate(self.xs1(h)):
            one.wait_recv()
        for way in (0, 1):
            to = p.at_x(1 if way == 0 else -1)

            def add(k, _):
                q, kk = 2 * way + k // p.nz, k % p.nz
                total = wide(self.part[h, to, q, kk]) + wide(self.x1[h, way, k // p.nz, kk])
                self.part[h, to, q, kk] = total.astype(jnp.bfloat16)
                return 0

            lax.fori_loop(0, 2 * p.nz, add, 0)
            self.xs2(h)[way].start()

    def s3(self, h):
        p = self.p
        for one in self.xs2(h):
            one.wait_recv()

        def add(k, _):
            q, kk = k // p.nz, k % p.nz
            total = wide(self.part[h, p.x, q, kk]) + (wide(self.x2[h, 0, q, kk]) + wide(self.x2[h, 1, q, kk]))
            self.yb[h, q, kk] = total.astype(jnp.bfloat16)
            return 0

        lax.fori_loop(0, RING * p.nz, add, 0)
        for one in self.ys1(h):
            one.start()

    def s4(self, h):
        p, half = self.p, self.p.nz // 2
        for one in self.ys1(h):
            one.wait_recv()
        for way in (0, 1):
            to = p.at_y(1 if way == 0 else -1)
            for k in range(half):
                kk = way * half + k
                self.yb[h, to, kk] = (wide(self.yb[h, to, kk]) + wide(self.y1[h, way, k])).astype(jnp.bfloat16)
            self.ys2(h)[way].start()

    def s5(self, h):
        p = self.p
        for one in self.ys2(h):
            one.wait_recv()
        for k in range(p.nz):
            total = wide(self.yb[h, p.y, k]) + (wide(self.y2[h, 0, k]) + wide(self.y2[h, 1, k]))
            self.zb[h, k] = total.astype(jnp.bfloat16)
        for d in range(1, p.nz):
            self.zs(h, d).start()

    def s6(self, h):
        p = self.p
        total = wide(self.zb[h, p.z])
        for d in range(1, p.nz):
            self.zs_from(h, d).wait_recv()
            total += wide(self.zr[h, p.at_z(d)])
        self.out[h, p.y, p.z] = total.astype(jnp.bfloat16)
        for d in range(1, p.nz):
            self.za(h, d).start()

    def s7(self, h):
        for d in range(1, self.p.nz):
            self.za_from(h, d).wait_recv()
        for one in self.ya1(h):
            one.start()

    def s8(self, h):
        p = self.p
        for one in self.ya1_from(h):
            one.wait_recv()
        for one in self.ya2(h, p.at_y(-1), p.at_y(1)):
            one.start()

    def s9(self, h):
        p = self.p
        for one in self.ya2(h, p.at_y(2), p.at_y(2)):
            one.wait_recv()
        self.finish(h)

    def drain(self, h):
        p = self.p
        for one in self.xs1(h) + self.xs2(h) + self.ys1(h) + self.ys2(h):
            one.wait_send()
        for d in range(1, p.nz):
            self.zs(h, d).wait_send()
            self.za(h, d).wait_send()
        for one in self.ya1(h) + self.ya2(h, p.at_y(-1), p.at_y(1)):
            one.wait_send()

    def unpack(self, h, b, unit, outs):
        for q in range(RING):
            for k, (rows, columns) in enumerate(self.gate[q]):
                for i in (0, 1):
                    for c in range(columns.start, columns.stop, unit):
                        to = pl.ds(pl.multiple_of(2 * c + b * unit, min(unit, 128)), min(unit, 128))
                        part = slice(c - columns.start, c - columns.start + unit)
                        outs[i][rows, to] = self.out[h, q, k, 16 * i : 16 * i + 16, part]
            for k, (rows, columns) in enumerate(self.down[q]):
                to = pl.ds(pl.multiple_of(b * self.down_rows + rows.start, 16), 16)
                outs[2][to, columns] = self.out[h, q, k, 32:48, :]


def nt(a, b):
    return lax.dot_general(a, b, (((1,), (1,)), ((), ())), preferred_element_type=jnp.float32)


def nn(a, b):
    return jnp.dot(a, b, preferred_element_type=jnp.float32)


def scaled(h):
    w = wide(h)
    return w, lax.rsqrt(jnp.mean(w * w, -1, keepdims=True) + 1e-6)


class Compute:
    def __init__(self, bufs, block):
        (self.wg, self.wu, self.wd, self.h, self.dy, self.dyt, self.a, self.at, self.acc, self.act, self.dg, self.du) = bufs
        self.block = block
        self.tokens, self.d = self.h.shape
        self.unit = self.wg.shape[3] // 16

    def each(self, body):
        def go(i, _):
            body(i, pl.ds(pl.multiple_of(i * self.block, self.block), self.block))
            return 0

        lax.fori_loop(0, self.tokens // self.block, go, 0)

    def enter(self, rows):
        w, scale = scaled(self.h[rows, :])
        self.a[0, rows, :] = (w * scale).astype(jnp.bfloat16)

    def turn_dy(self, rows):
        self.dyt[:, rows] = self.dy[rows, :].T

    def turn_a(self, l, rows):
        self.at[:, rows] = self.a[l, rows, :].T

    def forward(self, rows):
        a = self.a[0, rows, :]
        total = jnp.zeros((self.block, self.d), jnp.float32)
        ff = 16 * self.unit
        for j in range(4):
            cut = slice(j * ff // 4, (j + 1) * ff // 4)
            gate = nn(a, self.wg[0, :, :, cut].reshape(self.d, -1))
            up = nn(a, self.wu[0, :, :, cut].reshape(self.d, -1))
            act = (gate * lax.logistic(gate) * up).astype(jnp.bfloat16)
            total += nn(act, self.wd[0, 2 * j : 2 * j + 2].reshape(-1, self.d))
        h = self.h[rows, :] + total.astype(jnp.bfloat16)
        self.h[rows, :] = h
        w, scale = scaled(h)
        a = (w * scale).astype(jnp.bfloat16)
        self.a[1, rows, :] = a
        self.at[:, rows] = a.T

    def tile(self, l, b, x, gate_to, up_to, down_to):
        u = self.unit
        cuts = [pl.ds(pl.multiple_of((2 * x + c) * 2 * u + b * u, min(u, 128)), u) for c in (0, 1)]
        wg, wu = (
            jnp.concatenate([w[l, :, :, cut].reshape(self.d, u) for cut in cuts], axis=1) for w in (self.wg, self.wu)
        )
        wd = self.wd[l, pl.ds(2 * x, 2), pl.ds(pl.multiple_of(b * u, min(u, 128)), u), :].reshape(2 * u, self.d)

        def tokens(i, rows):
            a, dy = self.a[l, rows, :], self.dy[rows, :]
            gate, up, dact = nn(a, wg), nn(a, wu), nt(dy, wd)
            dact = wide(dact.astype(jnp.bfloat16))
            sig = lax.logistic(gate)
            silu = gate * sig
            dg = (dact * up * (sig + silu * (1 - sig))).astype(jnp.bfloat16)
            du = (dact * silu).astype(jnp.bfloat16)
            self.act[rows, :] = (silu * up).astype(jnp.bfloat16)
            self.dg[rows, :] = dg
            self.du[rows, :] = du
            if l == 1:
                self.acc[rows, :] += nt(dg, wg) + nt(du, wu)

        self.each(tokens)
        at = self.at[...]
        for from_, to in ((self.dg, gate_to), (self.du, up_to)):
            to[:, :, :, pl.ds(pl.multiple_of(2 * x * u, min(2 * u, 128)), 2 * u)] = (
                nn(at, from_[...]).astype(jnp.bfloat16).reshape(RING, 2, self.d // 8, 2 * u)
            )
        down_to[x] = nn(self.dyt[...], self.act[...]).T.astype(jnp.bfloat16).reshape(2, u, self.d)

    def back(self, rows):
        w, scale = scaled(self.h[rows, :])
        da = wide(self.acc[rows, :].astype(jnp.bfloat16))
        dot = jnp.sum(da * w, -1, keepdims=True) * (1.0 / self.d)
        dh = da * scale - w * (scale * scale * scale * dot)
        dy = self.dy[rows, :] + dh.astype(jnp.bfloat16)
        self.dy[rows, :] = dy
        self.dyt[:, rows] = dy.T
        self.at[:, rows] = self.a[0, rows, :].T


AFTER = (0, 1, 3, 6, 7, 8, 9, 10, 11, 12)


def step_kernel(nz, block, gate_block, down_block, *refs):
    x_in, dy_in, *rest = refs
    shards, outs, rest = rest[:3], rest[3:6], rest[6:]
    bufs, (own_g, own_d), reds, (snd, rcv, loc, io) = rest[:12], rest[12:14], rest[14:28], rest[28:]
    p = Place(nz)
    comp = Compute(bufs, block)
    unit, chunks = comp.unit, 4

    def own(h):
        return (
            lambda core: own_g.at[h % 2, 0, :, core],
            lambda core: own_g.at[h % 2, 1, :, core],
            lambda core: own_d.at[h % 2, :, core],
        )

    def finish(h):
        l, b = 1 - h // 2, h % 2
        red.unpack(h, b, unit, [o.at[l] for o in outs])

    red = Reduce(p, reds, own, gate_block, down_block, finish)
    gat = Gather(p, shards, bufs[:3], snd, rcv, loc)
    into = [pltpu.make_async_copy(x_in, comp.h, io.at[0]), pltpu.make_async_copy(dy_in, comp.dy, io.at[1])]
    for one in into:
        one.start()
    meet(red.peers())
    for i in range(3):
        gat.first(0, i)
    into[0].wait()
    comp.each(lambda i, rows: comp.enter(rows))
    gat.second(0, 0)
    into[1].wait()
    comp.each(lambda i, rows: comp.turn_dy(rows))
    gat.second(0, 1)
    gat.second(0, 2)
    for i in range(3):
        gat.first(1, i)
    for i in range(3):
        gat.third(0, i)
    for i in range(3):
        gat.last(0, i)
    comp.acc[...] = jnp.zeros_like(comp.acc)

    def ahead(i, rows):
        comp.forward(rows)
        for j in range(3):
            pl.when(i == j + 1)(functools.partial(gat.second, 1, j))

    comp.each(ahead)
    for i in range(3):
        gat.third(1, i)
    for i in range(3):
        gat.last(1, i)

    def tick(t):
        for k, (stage, after) in enumerate(zip(red.stages, AFTER, strict=True)):
            at = t - 3 - after
            pl.when((at >= 0) & (at < 4 * chunks) & (at % 4 == 0))(lambda stage=stage, at=at: stage(at // 4))

    for l in (1, 0):

        def tile(n, _):
            h = n // 4
            slot = h % 2
            comp.tile(l, n // 4 - 2 * (1 - l), n % 4, own_g.at[slot, 0], own_g.at[slot, 1], own_d.at[slot])
            tick(n)
            return 0

        lax.fori_loop(8 * (1 - l), 8 * (2 - l), tile, 0)
        if l == 1:
            comp.each(lambda i, rows: comp.back(rows))

    def late(t, _):
        tick(t)
        return 0

    lax.fori_loop(16, 16 + AFTER[-1], late, 0)

    def drain(h, _):
        red.drain(h)
        return 0

    lax.fori_loop(0, chunks, drain, 0)
    for l in (0, 1):
        for i in range(3):
            gat.drain(l, i)


def compute_scratch(tokens, d, ff):
    unit = ff // 16
    bf = jnp.bfloat16
    return [
        pltpu.VMEM((2, 8, d // 8, ff), bf),
        pltpu.VMEM((2, 8, d // 8, ff), bf),
        pltpu.VMEM((2, 8, ff // 8, d), bf),
        pltpu.VMEM((tokens, d), bf),
        pltpu.VMEM((tokens, d), bf),
        pltpu.VMEM((d, tokens), bf),
        pltpu.VMEM((2, tokens, d), bf),
        pltpu.VMEM((d, tokens), bf),
        pltpu.VMEM((tokens, d), jnp.float32),
        pltpu.VMEM((tokens, 2 * unit), bf),
        pltpu.VMEM((tokens, 2 * unit), bf),
        pltpu.VMEM((tokens, 2 * unit), bf),
    ]


def gradients_of(mesh, x, dy, weights):
    nz = mesh.shape["r"] // RING
    tokens, d = x.shape
    ff = weights[0].shape[2]
    gate_block, down_block = (d // 8, ff // 2), (ff // 16, d)
    any_space, vmem = pl.BlockSpec(memory_space=pl.ANY), pl.BlockSpec(memory_space=pltpu.VMEM)
    return pl.pallas_call(
        functools.partial(step_kernel, nz, min(512, tokens // 4), gate_block, down_block),
        out_shape=[jax.ShapeDtypeStruct(w.shape, w.dtype) for w in weights],
        in_specs=[any_space] * 5,
        out_specs=[vmem] * 3,
        scratch_shapes=compute_scratch(tokens, d, ff)
        + [
            pltpu.VMEM((2, 2, RING, 2) + gate_block, jnp.bfloat16),
            pltpu.VMEM((2, RING, 2) + down_block, jnp.bfloat16),
        ]
        + reduce_scratch(nz, 4, gate_block, down_block)
        + [
            pltpu.SemaphoreType.DMA((6, 9)),
            pltpu.SemaphoreType.DMA((6, 9)),
            pltpu.SemaphoreType.DMA((6,)),
            pltpu.SemaphoreType.DMA((2,)),
        ],
        compiler_params=pltpu.CompilerParams(collective_id=0, has_side_effects=True, vmem_limit_bytes=67043328),
        name="step",
    )(x, dy, *weights)


def solution(mesh):
    def step(x, dy, *arrays):
        weights, m, v = (arrays[i : i + 3] for i in (0, 3, 6))
        gradients = [g.astype(jnp.float32) for g in gradients_of(mesh, x[0], dy[0], weights)]
        new = [adamw(w.astype(jnp.float32), m, v, g) for w, m, v, g in zip(weights, m, v, gradients, strict=True)]
        return tuple(one[which] for which in range(3) for one in new)

    states, cut = P(("rep", "r", "s"), None, None), P(None, "s", None)
    return jax.shard_map(
        step,
        mesh=mesh,
        in_specs=(states, states) + (cut,) * 9,
        out_specs=(P("rep", "s", None),) * 9,
        check_vma=False,
    )
```

```python
import functools

import jax
import jax.numpy as jnp
from jax import lax
from jax.experimental import pallas as pl
from jax.experimental.pallas import tpu as pltpu
from jax.sharding import PartitionSpec as P

NAMES = ("w_gate", "w_up", "w_down")
MESH = pl.DeviceIdType.MESH
RING = 4
WAYS = (0, 1)
SPREAD = (1, 2)


def adamw(w, m, v, g):
    m = 0.9 * m + 0.1 * g
    v = 0.95 * v + 0.05 * g * g
    step = m * lax.rsqrt(v + 1e-8) + 0.1 * w
    return (w - 0.02 * step).astype(jnp.bfloat16), m, v


class Place:
    def __init__(self, nz):
        self.nz = nz
        r, s = lax.axis_index("r"), lax.axis_index("s")
        self.y, self.z, self.x, self.core, self.s, self.r = r // nz, r % nz, s // 2, s % 2, s, r
        self.partner = {"s": 2 * self.x + 1 - self.core}
        self.right, self.left, self.above, self.below = self.to_x(1), self.to_x(-1), self.to_y(1), self.to_y(-1)
        self.x_right, self.x_left, self.x_far = (self.at_x(d) for d in (1, -1, 2))
        self.y_above, self.y_below, self.y_far = (self.at_y(d) for d in (1, -1, 2))

    def at_x(self, d):
        return (self.x + d) % RING

    def at_y(self, d):
        return (self.y + d) % RING

    def at_z(self, d):
        return (self.z + d) % self.nz

    def to_x(self, d):
        return {"s": 2 * self.at_x(d) + self.core}

    def to_y(self, d):
        return {"r": self.at_y(d) * self.nz + self.z}

    def to_z(self, d):
        return {"r": self.y * self.nz + self.at_z(d)}


def loop(stop, body, start=0):
    def go(i, carry):
        body(i, carry)
        return carry

    lax.fori_loop(start, stop, go, 0)


def meet(peers):
    barrier = pltpu.get_barrier_semaphore()
    for peer in peers:
        pl.semaphore_signal(barrier, inc=1, device_id=peer, device_id_type=MESH)
    pl.semaphore_wait(barrier, len(peers))


def send(src, dst, sems, device):
    send_sem, recv_sem = sems
    return pltpu.make_async_remote_copy(
        src_ref=src, dst_ref=dst, send_sem=send_sem, recv_sem=recv_sem, device_id=device, device_id_type=MESH
    )


class Gather:
    def __init__(self, p, ins, outs, snd, rcv, loc):
        self.p, self.ins, self.outs, self.snd, self.rcv, self.loc = p, ins, outs, snd, rcv, loc

    def block(self, l, i, x, half=None):
        ref = self.outs[i].at[l, 2 * x + self.p.core]
        if half is None:
            return ref
        rows = ref.shape[0] // 2
        return ref.at[pl.ds(half * rows, rows)]

    def copy(self, l, i, k, src, dst, device):
        return send(src, dst, (self.snd.at[3 * l + i, k], self.rcv.at[3 * l + i, k]), device)

    def own(self, l, i, k):
        p = self.p
        return self.copy(l, i, k, self.ins[i].at[l], self.block(l, i, p.x), (p.right, p.left, p.partner)[k])

    def local(self, l, i):
        return pltpu.make_async_copy(self.ins[i].at[l], self.block(l, i, self.p.x), self.loc.at[3 * l + i])

    def on(self, l, i, k):
        p = self.p
        b = self.block(l, i, (p.x_left, p.x_right)[k], k)
        return self.copy(l, i, 3 + k, b, b, (p.right, p.left)[k])

    def over(self, l, i, k):
        p = self.p
        b = self.block(l, i, (p.x_left, p.x_right, p.x_far, p.x_far)[k], (None, None, 0, 1)[k])
        return self.copy(l, i, 5 + k, b, b, p.partner)

    def first(self, l, i):
        self.local(l, i).start()
        for k in range(3):
            self.own(l, i, k).start()

    def second(self, l, i):
        for k in WAYS:
            self.own(l, i, k).wait_recv()
            self.on(l, i, k).start()
            self.over(l, i, k).start()

    def third(self, l, i):
        for k in WAYS:
            self.on(l, i, k).wait_recv()
            self.over(l, i, 2 + k).start()

    def last(self, l, i):
        self.own(l, i, 2).wait_recv()
        for k in range(4):
            self.over(l, i, k).wait_recv()
        self.local(l, i).wait()

    def drain(self, l, i):
        for k in range(3):
            self.own(l, i, k).wait_send()
        for k in WAYS:
            self.on(l, i, k).wait_send()
        for k in range(4):
            self.over(l, i, k).wait_send()


def pieces(rows, columns, by_rows):
    qr, qc = (rows // RING, columns) if by_rows else (rows, columns // RING)
    across = qc // 128
    return [
        [
            (slice((q * qr if by_rows else 0) + 16 * (k // across), (q * qr if by_rows else 0) + 16 * (k // across) + 16),
             slice((0 if by_rows else q * qc) + 128 * (k % across), (0 if by_rows else q * qc) + 128 * (k % across) + 128))
            for k in range(qr // 16 * across)
        ]
        for q in range(RING)
    ]


def wide(ref):
    return ref.astype(jnp.float32)


SCRATCH = ("dg", "dd", "part", "x1", "x2", "yb", "y1", "y2", "zb", "zr", "out", "sem_d", "sem_l", "sem_z")


def reduce_scratch(nz, chunks, gate_block, down_block):
    bf = functools.partial(pltpu.VMEM, dtype=jnp.bfloat16)
    piece = (48, 128)
    return [
        pltpu.VMEM((2, 2, RING) + gate_block, jnp.bfloat16),
        pltpu.VMEM((2, RING) + down_block, jnp.bfloat16),
        pltpu.VMEM((2, RING, RING, nz) + piece, jnp.bfloat16),
        pltpu.VMEM((chunks, 2, RING // 2, nz) + piece, jnp.bfloat16),
        pltpu.VMEM((chunks, 2, RING, nz) + piece, jnp.bfloat16),
        pltpu.VMEM((chunks, RING, nz) + piece, jnp.bfloat16),
        pltpu.VMEM((chunks, 2, nz // 2) + piece, jnp.bfloat16),
        pltpu.VMEM((chunks, 2, nz) + piece, jnp.bfloat16),
        pltpu.VMEM((chunks, nz) + piece, jnp.bfloat16),
        pltpu.VMEM((chunks, nz) + piece, jnp.bfloat16),
        pltpu.VMEM((chunks, RING, nz) + piece, jnp.bfloat16),
        pltpu.SemaphoreType.DMA((2, chunks, 3)),
        pltpu.SemaphoreType.DMA((2, chunks, 6, 2)),
        pltpu.SemaphoreType.DMA((2, chunks, 2, nz)),
    ]


class Reduce:
    def __init__(self, p, bufs, own, gate_block, down_block, finish):
        self.p, self.own, self.finish = p, own, finish
        for name, ref in zip(SCRATCH, bufs, strict=True):
            setattr(self, name, ref)
        self.down_rows = down_block[0]
        self.gate, self.down = pieces(*gate_block, False), pieces(*down_block, True)
        self.stages = [self.s0, self.s1, self.s2, self.s3, self.s4, self.s5, self.s6, self.s7, self.s8, self.s9]

    def peers(self):
        p = self.p
        return [p.partner, p.right, p.left, p.above, p.below] + [p.to_z(d) for d in range(1, p.nz)]

    def link(self, h, k, way, src, dst, device):
        return send(src, dst, (self.sem_l.at[0, h, k, way], self.sem_l.at[1, h, k, way]), device)

    def d2d(self, h, core):
        own = self.own(h)
        dst = [self.dg.at[h % 2, 0], self.dg.at[h % 2, 1], self.dd.at[h % 2]]
        return [
            send(own[i](core), dst[i], (self.sem_d.at[0, h, i], self.sem_d.at[1, h, i]), self.p.partner) for i in range(3)
        ]

    def s0(self, h):
        for one in self.d2d(h, 1 - self.p.core):
            one.start()

    def xs1(self, h):
        p = self.p
        block = self.part.at[h % 2, p.x_far]
        return [
            self.link(h, 0, 0, block.at[pl.ds(0, 2)], self.x1.at[h, 0], p.right),
            self.link(h, 0, 1, block.at[pl.ds(2, 2)], self.x1.at[h, 1], p.left),
        ]

    def xs2(self, h):
        p = self.p
        return [
            self.link(h, 1, 0, self.part.at[h % 2, p.x_right], self.x2.at[h, 0], p.right),
            self.link(h, 1, 1, self.part.at[h % 2, p.x_left], self.x2.at[h, 1], p.left),
        ]

    def ys1(self, h):
        p = self.p
        block, half = self.yb.at[h, p.y_far], p.nz // 2
        return [
            self.link(h, 2, 0, block.at[pl.ds(0, half)], self.y1.at[h, 0], p.above),
            self.link(h, 2, 1, block.at[pl.ds(half, half)], self.y1.at[h, 1], p.below),
        ]

    def ys2(self, h):
        p = self.p
        return [
            self.link(h, 3, 0, self.yb.at[h, p.y_above], self.y2.at[h, 0], p.above),
            self.link(h, 3, 1, self.yb.at[h, p.y_below], self.y2.at[h, 1], p.below),
        ]

    def zs(self, h, d):
        p = self.p
        to = p.at_z(d)
        return send(self.zb.at[h, to], self.zr.at[h, p.z], (self.sem_z.at[0, h, 0, to], self.sem_z.at[1, h, 0, p.z]), p.to_z(d))

    def zs_from(self, h, d):
        p = self.p
        src = p.at_z(d)
        return send(self.zb.at[h, src], self.zr.at[h, src], (self.sem_z.at[0, h, 0, src], self.sem_z.at[1, h, 0, src]), p.to_z(d))

    def za(self, h, d):
        p = self.p
        mine = self.out.at[h, p.y, p.z]
        return send(mine, mine, (self.sem_z.at[0, h, 1, p.at_z(d)], self.sem_z.at[1, h, 1, p.z]), p.to_z(d))

    def za_from(self, h, d):
        p = self.p
        src = p.at_z(d)
        piece = self.out.at[h, p.y, src]
        return send(piece, piece, (self.sem_z.at[0, h, 1, src], self.sem_z.at[1, h, 1, src]), p.to_z(d))

    def ya1(self, h, y=None):
        p = self.p
        piece = self.out.at[h, p.y]
        return [self.link(h, 4, 0, piece, piece, p.above), self.link(h, 4, 1, piece, piece, p.below)]

    def ya1_from(self, h):
        p = self.p
        below, above = self.out.at[h, p.y_below], self.out.at[h, p.y_above]
        return [self.link(h, 4, 0, below, below, p.above), self.link(h, 4, 1, above, above, p.below)]

    def ya2(self, h, first, second):
        p, half = self.p, self.p.nz // 2
        a, b = self.out.at[h, first, pl.ds(0, half)], self.out.at[h, second, pl.ds(half, half)]
        return [self.link(h, 5, 0, a, a, p.above), self.link(h, 5, 1, b, b, p.below)]

    def s1(self, h):
        p = self.p
        for one in self.d2d(h, 1 - p.core):
            one.wait_recv()
            one.wait_send()
        own = self.own(h)

        def block(x, _):
            for i, cut in ((0, self.gate), (1, self.gate), (2, self.down)):
                mine = own[i](p.core).at[x]
                theirs = self.dd.at[h % 2, x] if i == 2 else self.dg.at[h % 2, i, x]
                for q in range(RING):
                    for k, (rows, columns) in enumerate(cut[q]):
                        total = wide(mine[rows, columns]) + wide(theirs[rows, columns])
                        self.part[h % 2, x, q, k, 16 * i : 16 * i + 16, :] = total.astype(jnp.bfloat16)

        loop(RING, block)
        for one in self.xs1(h):
            one.start()

    def s2(self, h):
        p = self.p
        for way, one in enumerate(self.xs1(h)):
            one.wait_recv()
        for way in WAYS:
            to = (p.x_right, p.x_left)[way]

            def add(k, _):
                q, kk = 2 * way + k // p.nz, k % p.nz
                total = wide(self.part[h % 2, to, q, kk]) + wide(self.x1[h, way, k // p.nz, kk])
                self.part[h % 2, to, q, kk] = total.astype(jnp.bfloat16)

            loop(2 * p.nz, add)
            self.xs2(h)[way].start()

    def s3(self, h):
        p = self.p
        for one in self.xs2(h):
            one.wait_recv()
        for one in self.xs1(h) + self.xs2(h):
            one.wait_send()

        def add(k, _):
            q, kk = k // p.nz, k % p.nz
            total = wide(self.part[h % 2, p.x, q, kk]) + (wide(self.x2[h, 0, q, kk]) + wide(self.x2[h, 1, q, kk]))
            self.yb[h, q, kk] = total.astype(jnp.bfloat16)

        loop(RING * p.nz, add)
        for one in self.ys1(h):
            one.start()

    def s4(self, h):
        p, half = self.p, self.p.nz // 2
        for one in self.ys1(h):
            one.wait_recv()
        for way in WAYS:
            to = (p.y_above, p.y_below)[way]
            for k in range(half):
                kk = way * half + k
                self.yb[h, to, kk] = (wide(self.yb[h, to, kk]) + wide(self.y1[h, way, k])).astype(jnp.bfloat16)
            self.ys2(h)[way].start()

    def s5(self, h):
        p = self.p
        for one in self.ys2(h):
            one.wait_recv()
        for k in range(p.nz):
            total = wide(self.yb[h, p.y, k]) + (wide(self.y2[h, 0, k]) + wide(self.y2[h, 1, k]))
            self.zb[h, k] = total.astype(jnp.bfloat16)
        for d in range(1, p.nz):
            self.zs(h, d).start()

    def s6(self, h):
        p = self.p
        total = wide(self.zb[h, p.z])
        for d in range(1, p.nz):
            self.zs_from(h, d).wait_recv()
            total += wide(self.zr[h, p.at_z(d)])
        self.out[h, p.y, p.z] = total.astype(jnp.bfloat16)
        for d in range(1, p.nz):
            self.za(h, d).start()

    def s7(self, h):
        for d in range(1, self.p.nz):
            self.za_from(h, d).wait_recv()
        for one in self.ya1(h):
            one.start()

    def s8(self, h):
        p = self.p
        for one in self.ya1_from(h):
            one.wait_recv()
        for one in self.ya2(h, p.y_below, p.y_above):
            one.start()

    def s9(self, h):
        p = self.p
        for one in self.ya2(h, p.y_far, p.y_far):
            one.wait_recv()
        self.finish(h)

    def drain(self, h):
        p = self.p
        for one in self.ys1(h) + self.ys2(h):
            one.wait_send()
        for d in range(1, p.nz):
            self.zs(h, d).wait_send()
            self.za(h, d).wait_send()
        for one in self.ya1(h) + self.ya2(h, p.y_below, p.y_above):
            one.wait_send()

    def unpack(self, h, b, unit, outs):
        for q in range(RING):
            for k, (rows, columns) in enumerate(self.gate[q]):
                for i in (0, 1):
                    for c in range(columns.start, columns.stop, unit):
                        to = pl.ds(pl.multiple_of(2 * c + b * unit, min(unit, 128)), min(unit, 128))
                        part = slice(c - columns.start, c - columns.start + unit)
                        outs[i][rows, to] = self.out[h, q, k, 16 * i : 16 * i + 16, part]
            for k, (rows, columns) in enumerate(self.down[q]):
                to = pl.ds(pl.multiple_of(b * self.down_rows + rows.start, 16), 16)
                outs[2][to, columns] = self.out[h, q, k, 32:48, :]


class Spread:
    def __init__(self, p, ins, outs, snd, rcv, loc):
        self.p, self.ins, self.outs, self.snd, self.rcv, self.loc = p, ins, outs, snd, rcv, loc

    def block(self, l, i, x, y=None, half=None):
        ref = self.outs[i].at[l, 2 * x + self.p.core]
        return ref if y is None else self.part(ref, y, half)

    def part(self, ref, y, half=None):
        rows, columns = ref.shape[0] // RING, ref.shape[1] // 2
        some = pl.ds(pl.multiple_of(y * rows, rows), rows)
        return ref.at[some] if half is None else ref.at[some, pl.ds(half * columns, columns)]

    def copy(self, l, i, k, src, dst, device):
        n = 2 * l + i - 1
        return send(src, dst, (self.snd.at[n, k], self.rcv.at[n, k]), device)

    def local(self, l, i):
        return pltpu.make_async_copy(self.ins[i].at[l], self.block(l, i, self.p.x), self.loc.at[3 * l + i])

    def own(self, l, i):
        return self.copy(l, i, 0, self.ins[i].at[l], self.block(l, i, self.p.x), self.p.partner)

    def x1(self, l, i, way):
        p = self.p
        src = self.part(self.ins[i].at[l], p.y)
        return self.copy(l, i, 1 + way, src, self.block(l, i, p.x, p.y), (p.right, p.left)[way])

    def x2(self, l, i, way):
        p = self.p
        b = self.block(l, i, (p.x_left, p.x_right)[way], p.y, way)
        return self.copy(l, i, 3 + way, b, b, (p.right, p.left)[way])

    def y1(self, l, i, n, way):
        p = self.p
        b = self.block(l, i, p.at_x(n + 1), p.y)
        return self.copy(l, i, 5 + 2 * n + way, b, b, (p.above, p.below)[way])

    def y2(self, l, i, n, way):
        p = self.p
        b = self.block(l, i, p.at_x(n + 1), (p.y_below, p.y_above)[way], way)
        return self.copy(l, i, 11 + 2 * n + way, b, b, (p.above, p.below)[way])

    def over(self, l, i, n):
        b = self.block(l, i, self.p.at_x(n + 1))
        return self.copy(l, i, 17 + n, b, b, self.p.partner)

    def f1(self, l, i):
        for way in WAYS:
            self.x1(l, i, way).start()
        self.local(l, i).start()
        self.own(l, i).start()

    def f2(self, l, i):
        for way in WAYS:
            self.x1(l, i, way).wait_recv()
            self.x2(l, i, way).start()
            for to in (0, 1):
                self.y1(l, i, (2, 0)[way], to).start()

    def f3(self, l, i):
        for way in WAYS:
            self.x2(l, i, way).wait_recv()
        for to in (0, 1):
            self.y1(l, i, 1, to).start()

    def f4(self, l, i):
        def go(n, _):
            for way in WAYS:
                self.y1(l, i, (n + 2) % 3, way).wait_recv()
                self.y2(l, i, (n + 2) % 3, way).start()

        loop(3, go)

    def f5(self, l, i):
        def go(n, _):
            for way in WAYS:
                self.y2(l, i, (n + 2) % 3, way).wait_recv()
            self.over(l, i, (n + 2) % 3).start()

        loop(3, go)

    def f6(self, l, i):
        self.local(l, i).wait()
        self.own(l, i).wait_recv()

        def go(n, _):
            self.over(l, i, n).wait_recv()

        loop(3, go)

    def drain(self, l, i):
        self.own(l, i).wait_send()
        for way in WAYS:
            self.x1(l, i, way).wait_send()
            self.x2(l, i, way).wait_send()

        def go(n, _):
            for way in WAYS:
                self.y1(l, i, n, way).wait_send()
                self.y2(l, i, n, way).wait_send()
            self.over(l, i, n).wait_send()

        loop(3, go)


def nt(a, b):
    return lax.dot_general(a, b, (((1,), (1,)), ((), ())), preferred_element_type=jnp.float32)


def nn(a, b):
    return jnp.dot(a, b, preferred_element_type=jnp.float32)


def scaled(h):
    w = wide(h)
    return w, lax.rsqrt(jnp.mean(w * w, -1, keepdims=True) + 1e-6)


class Compute:
    def __init__(self, bufs, block):
        (self.wg, self.wu, self.wd, self.h, self.dy, self.dyt, self.a, self.at, self.acc, self.act, self.dg, self.du, self.sums) = bufs
        self.block = block
        self.tokens, self.d = self.h.shape
        self.unit = self.wg.shape[3] // 16

    def each(self, body):
        def go(i, _):
            body(i, pl.ds(pl.multiple_of(i * self.block, self.block), self.block))

        loop(self.tokens // self.block, go)

    def enter(self, rows):
        w, scale = scaled(self.h[rows, :])
        self.a[0, rows, :] = (w * scale).astype(jnp.bfloat16)

    def turn_dy(self, rows):
        self.dyt[:, rows] = self.dy[rows, :].T

    def turn_a(self, l, rows):
        self.at[:, rows] = self.a[l, rows, :].T

    def forward(self, rows):
        a = self.a[0, rows, :]
        total = jnp.zeros((self.block, self.d), jnp.float32)
        ff = 16 * self.unit
        for j in range(4):
            cut = slice(j * ff // 4, (j + 1) * ff // 4)
            gate = nn(a, self.wg[0, :, :, cut].reshape(self.d, -1))
            up = nn(a, self.wu[0, :, :, cut].reshape(self.d, -1))
            act = (gate * lax.logistic(gate) * up).astype(jnp.bfloat16)
            total += nn(act, self.wd[0, 2 * j : 2 * j + 2].reshape(-1, self.d))
        h = self.h[rows, :] + total.astype(jnp.bfloat16)
        self.h[rows, :] = h
        w, scale = scaled(h)
        a = (w * scale).astype(jnp.bfloat16)
        self.a[1, rows, :] = a
        self.at[:, rows] = a.T

    def tile(self, l, n, last=None):
        u = self.unit
        b, x, slot = n // 4, n % 4, n % 2
        cuts = [pl.ds(pl.multiple_of((2 * x + c) * 2 * u + b * u, min(u, 128)), u) for c in (0, 1)]
        wg, wu = (
            jnp.concatenate([w[l, :, :, cut].reshape(self.d, u) for cut in cuts], axis=1) for w in (self.wg, self.wu)
        )
        wd = self.wd[l, pl.ds(2 * x, 2), pl.ds(pl.multiple_of(b * u, min(u, 128)), u), :].reshape(2 * u, self.d)

        def tokens(i, rows):
            a, dy = self.a[l, rows, :], self.dy[rows, :]
            gate, up, dact = nn(a, wg), nn(a, wu), nt(dy, wd)
            if last is not None:
                self.weigh(rows, 1 - slot)
            dact = wide(dact.astype(jnp.bfloat16))
            sig = lax.logistic(gate)
            silu = gate * sig
            dg = (dact * up * (sig + silu * (1 - sig))).astype(jnp.bfloat16)
            du = (dact * silu).astype(jnp.bfloat16)
            self.act[slot, rows, :] = (silu * up).astype(jnp.bfloat16)
            self.dg[slot, rows, :] = dg
            self.du[slot, rows, :] = du
            if l == 1:
                self.acc[rows, :] += nt(dg, wg) + nt(du, wu)

        self.each(tokens)
        if last is not None:
            self.settle((n - 1) % 4, *last)

    def weigh(self, rows, slot):
        for j, (left, right) in enumerate(((self.at, self.dg), (self.at, self.du), (self.dyt, self.act))):
            self.sums[j] += nn(left[:, rows], right[slot, rows, :])

    def settle(self, x, gate_to, up_to, down_to):
        u = self.unit
        columns = pl.ds(pl.multiple_of(2 * x * u, min(2 * u, 128)), 2 * u)
        for j, to in enumerate((gate_to, up_to)):
            to[:, :, :, columns] = self.sums[j].astype(jnp.bfloat16).reshape(RING, 2, self.d // 8, 2 * u)
        down_to[x] = self.sums[2].T.astype(jnp.bfloat16).reshape(2, u, self.d)
        self.sums[...] = jnp.zeros_like(self.sums)

    def back(self, rows):
        w, scale = scaled(self.h[rows, :])
        da = wide(self.acc[rows, :].astype(jnp.bfloat16))
        dot = jnp.sum(da * w, -1, keepdims=True) * (1.0 / self.d)
        dh = da * scale - w * (scale * scale * scale * dot)
        dy = self.dy[rows, :] + dh.astype(jnp.bfloat16)
        self.dy[rows, :] = dy
        self.dyt[:, rows] = dy.T
        self.at[:, rows] = self.a[0, rows, :].T


AFTER = (0, 1, 2, 5, 6, 7, 8, 9, 10, 11)


def step_kernel(nz, block, gate_block, down_block, *refs):
    x_in, dy_in, *rest = refs
    shards, outs, rest = rest[:3], rest[3:6], rest[6:]
    bufs, (own_g, own_d), reds, (snd, rcv, loc, io, snd_y, rcv_y) = rest[:13], rest[13:15], rest[15:29], rest[29:]
    p = Place(nz)
    comp = Compute(bufs, block)
    unit, chunks = comp.unit, 4

    def own(h):
        return (
            lambda core: own_g.at[h % 2, 0, :, core],
            lambda core: own_g.at[h % 2, 1, :, core],
            lambda core: own_d.at[h % 2, :, core],
        )

    def finish(h):
        l, b = 1 - h // 2, h % 2
        red.unpack(h, b, unit, [o.at[l] for o in outs])

    red = Reduce(p, reds, own, gate_block, down_block, finish)
    gat = Gather(p, shards, bufs[:3], snd, rcv, loc)
    spr = Spread(p, shards, bufs[:3], snd_y, rcv_y, loc)
    into = [pltpu.make_async_copy(x_in, comp.h, io.at[0]), pltpu.make_async_copy(dy_in, comp.dy, io.at[1])]
    for one in into:
        one.start()
    meet(red.peers())
    for i in SPREAD:
        spr.f1(0, i)
    into[0].wait()
    for i in SPREAD:
        spr.f2(0, i)
    gat.first(0, 0)
    comp.each(lambda i, rows: comp.enter(rows))
    for i in SPREAD:
        spr.f3(0, i)
    into[1].wait()
    comp.each(lambda i, rows: comp.turn_dy(rows))
    comp.acc[...] = jnp.zeros_like(comp.acc)
    comp.sums[...] = jnp.zeros_like(comp.sums)
    gat.second(0, 0)
    for i in SPREAD:
        spr.f4(0, i)
        spr.f1(1, i)
    gat.third(0, 0)
    for i in SPREAD:
        spr.f2(1, i)
    gat.first(1, 0)
    for i in SPREAD:
        spr.f5(0, i)
    gat.last(0, 0)
    for i in SPREAD:
        spr.f6(0, i)
    for i in SPREAD:
        spr.f3(1, i)

    def ahead(i, rows):
        comp.forward(rows)

        @pl.when(i == 0)
        def _():
            gat.second(1, 0)
            spr.f4(1, 1)

        @pl.when(i == 1)
        def _():
            spr.f4(1, 2)
            gat.third(1, 0)

        pl.when(i == 2)(lambda: spr.f5(1, 1))

    comp.each(ahead)
    spr.f5(1, 2)
    gat.last(1, 0)
    for i in SPREAD:
        spr.f6(1, i)

    def tick(t):
        for k, (stage, after) in enumerate(zip(red.stages, AFTER, strict=True)):
            since = t - 4 - after
            h = 2 * (since // 8) + (since % 8) // 3
            due = (since >= 0) & (since < 16) & ((since % 8 == 0) | (since % 8 == 3))
            pl.when(due)(lambda stage=stage, h=h: stage(h))

    def terms(n):
        slot = n // 4 % 2
        return own_g.at[slot, 0], own_g.at[slot, 1], own_d.at[slot]

    for l in (1, 0):
        base = 8 * (1 - l)
        comp.tile(l, 0)

        def tile(n, _):
            tick(base + n - 1)
            comp.tile(l, n, terms(n - 1))

        loop(8, tile, 1)
        comp.each(lambda i, rows: comp.weigh(rows, 1))
        comp.settle(3, *terms(7))
        tick(base + 7)
        if l == 1:
            comp.each(lambda i, rows: comp.back(rows))

    def late(t, _):
        tick(t)

    loop(16 + AFTER[-1], late, 16)

    def drain(h, _):
        red.drain(h)

    loop(chunks, drain)
    def rest(l, _):
        gat.drain(l, 0)
        for i in SPREAD:
            spr.drain(l, i)

    loop(2, rest)


def compute_scratch(tokens, d, ff):
    unit = ff // 16
    bf = jnp.bfloat16
    return [
        pltpu.VMEM((2, 8, d // 8, ff), bf),
        pltpu.VMEM((2, 8, d // 8, ff), bf),
        pltpu.VMEM((2, 8, ff // 8, d), bf),
        pltpu.VMEM((tokens, d), bf),
        pltpu.VMEM((tokens, d), bf),
        pltpu.VMEM((d, tokens), bf),
        pltpu.VMEM((2, tokens, d), bf),
        pltpu.VMEM((d, tokens), bf),
        pltpu.VMEM((tokens, d), jnp.float32),
        pltpu.VMEM((2, tokens, 2 * unit), bf),
        pltpu.VMEM((2, tokens, 2 * unit), bf),
        pltpu.VMEM((2, tokens, 2 * unit), bf),
        pltpu.VMEM((3, d, 2 * unit), jnp.float32),
    ]


def gradients_of(mesh, x, dy, weights):
    nz = mesh.shape["r"] // RING
    tokens, d = x.shape
    ff = weights[0].shape[2]
    gate_block, down_block = (d // 8, ff // 2), (ff // 16, d)
    any_space, vmem = pl.BlockSpec(memory_space=pl.ANY), pl.BlockSpec(memory_space=pltpu.VMEM)
    return pl.pallas_call(
        functools.partial(step_kernel, nz, min(512, tokens // 4), gate_block, down_block),
        out_shape=[jax.ShapeDtypeStruct(w.shape, w.dtype) for w in weights],
        in_specs=[any_space] * 5,
        out_specs=[vmem] * 3,
        scratch_shapes=compute_scratch(tokens, d, ff)
        + [
            pltpu.VMEM((2, 2, RING, 2) + gate_block, jnp.bfloat16),
            pltpu.VMEM((2, RING, 2) + down_block, jnp.bfloat16),
        ]
        + reduce_scratch(nz, 4, gate_block, down_block)
        + [
            pltpu.SemaphoreType.DMA((6, 9)),
            pltpu.SemaphoreType.DMA((6, 9)),
            pltpu.SemaphoreType.DMA((6,)),
            pltpu.SemaphoreType.DMA((2,)),
            pltpu.SemaphoreType.DMA((4, 20)),
            pltpu.SemaphoreType.DMA((4, 20)),
        ],
        compiler_params=pltpu.CompilerParams(collective_id=0, has_side_effects=True, vmem_limit_bytes=67043328),
        name="step",
    )(x, dy, *weights)


def solution(mesh):
    def step(x, dy, *arrays):
        weights, m, v = (arrays[i : i + 3] for i in (0, 3, 6))
        gradients = [g.astype(jnp.float32) for g in gradients_of(mesh, x[0], dy[0], weights)]
        new = [adamw(w.astype(jnp.float32), m, v, g) for w, m, v, g in zip(weights, m, v, gradients, strict=True)]
        return tuple(one[which] for which in range(3) for one in new)

    states, cut = P(("rep", "r", "s"), None, None), P(None, "s", None)
    return jax.shard_map(
        step,
        mesh=mesh,
        in_specs=(states, states) + (cut,) * 9,
        out_specs=(P("rep", "s", None),) * 9,
        check_vma=False,
    )
```

```python
import functools

import jax
import jax.numpy as jnp
from jax import lax
from jax.experimental import pallas as pl
from jax.experimental.pallas import tpu as pltpu
from jax.sharding import PartitionSpec as P

NAMES = ("w_gate", "w_up", "w_down")
MESH = pl.DeviceIdType.MESH
RING = 4
WAYS = (0, 1)
SPREAD = (1, 2)


def adamw(w, m, v, g):
    m = 0.9 * m + 0.1 * g
    v = 0.95 * v + 0.05 * g * g
    step = m * lax.rsqrt(v + 1e-8) + 0.1 * w
    return (w - 0.02 * step).astype(jnp.bfloat16), m, v


class Place:
    def __init__(self, nz):
        self.nz = nz
        r, s = lax.axis_index("r"), lax.axis_index("s")
        self.y, self.z, self.x, self.core, self.s, self.r = r // nz, r % nz, s // 2, s % 2, s, r
        self.partner = {"s": 2 * self.x + 1 - self.core}
        self.right, self.left, self.above, self.below = self.to_x(1), self.to_x(-1), self.to_y(1), self.to_y(-1)
        self.x_right, self.x_left, self.x_far = (self.at_x(d) for d in (1, -1, 2))
        self.y_above, self.y_below, self.y_far = (self.at_y(d) for d in (1, -1, 2))

    def at_x(self, d):
        return (self.x + d) % RING

    def at_y(self, d):
        return (self.y + d) % RING

    def at_z(self, d):
        return (self.z + d) % self.nz

    def to_x(self, d):
        return {"s": 2 * self.at_x(d) + self.core}

    def to_y(self, d):
        return {"r": self.at_y(d) * self.nz + self.z}

    def to_z(self, d):
        return {"r": self.y * self.nz + self.at_z(d)}


def loop(stop, body, start=0):
    def go(i, carry):
        body(i, carry)
        return carry

    lax.fori_loop(start, stop, go, 0)


def meet(peers):
    barrier = pltpu.get_barrier_semaphore()
    for peer in peers:
        pl.semaphore_signal(barrier, inc=1, device_id=peer, device_id_type=MESH)
    pl.semaphore_wait(barrier, len(peers))


def send(src, dst, sems, device):
    send_sem, recv_sem = sems
    return pltpu.make_async_remote_copy(
        src_ref=src, dst_ref=dst, send_sem=send_sem, recv_sem=recv_sem, device_id=device, device_id_type=MESH
    )


class Gather:
    def __init__(self, p, ins, outs, snd, rcv, loc):
        self.p, self.ins, self.outs, self.snd, self.rcv, self.loc = p, ins, outs, snd, rcv, loc

    def block(self, l, i, x, half=None):
        ref = self.outs[i].at[l, 2 * x + self.p.core]
        if half is None:
            return ref
        rows = ref.shape[0] // 2
        return ref.at[pl.ds(half * rows, rows)]

    def copy(self, l, i, k, src, dst, device):
        return send(src, dst, (self.snd.at[3 * l + i, k], self.rcv.at[3 * l + i, k]), device)

    def own(self, l, i, k):
        p = self.p
        return self.copy(l, i, k, self.ins[i].at[l], self.block(l, i, p.x), (p.right, p.left, p.partner)[k])

    def local(self, l, i):
        return pltpu.make_async_copy(self.ins[i].at[l], self.block(l, i, self.p.x), self.loc.at[3 * l + i])

    def on(self, l, i, k):
        p = self.p
        b = self.block(l, i, (p.x_left, p.x_right)[k], k)
        return self.copy(l, i, 3 + k, b, b, (p.right, p.left)[k])

    def over(self, l, i, k):
        p = self.p
        b = self.block(l, i, (p.x_left, p.x_right, p.x_far, p.x_far)[k], (None, None, 0, 1)[k])
        return self.copy(l, i, 5 + k, b, b, p.partner)

    def first(self, l, i):
        self.local(l, i).start()
        for k in range(3):
            self.own(l, i, k).start()

    def second(self, l, i):
        for k in WAYS:
            self.own(l, i, k).wait_recv()
            self.on(l, i, k).start()
            self.over(l, i, k).start()

    def third(self, l, i):
        for k in WAYS:
            self.on(l, i, k).wait_recv()
            self.over(l, i, 2 + k).start()

    def last(self, l, i):
        self.own(l, i, 2).wait_recv()
        for k in range(4):
            self.over(l, i, k).wait_recv()
        self.local(l, i).wait()

    def drain(self, l, i):
        for k in range(3):
            self.own(l, i, k).wait_send()
        for k in WAYS:
            self.on(l, i, k).wait_send()
        for k in range(4):
            self.over(l, i, k).wait_send()


def pieces(rows, columns, by_rows):
    qr, qc = (rows // RING, columns) if by_rows else (rows, columns // RING)
    across = qc // 128
    return [
        [
            (slice((q * qr if by_rows else 0) + 16 * (k // across), (q * qr if by_rows else 0) + 16 * (k // across) + 16),
             slice((0 if by_rows else q * qc) + 128 * (k % across), (0 if by_rows else q * qc) + 128 * (k % across) + 128))
            for k in range(qr // 16 * across)
        ]
        for q in range(RING)
    ]


def wide(ref):
    return ref.astype(jnp.float32)


SCRATCH = ("dg", "dd", "part", "x1", "x2", "yb", "y1", "y2", "zb", "zr", "out", "sem_d", "sem_l", "sem_z")


def reduce_scratch(nz, chunks, gate_block, down_block):
    bf = functools.partial(pltpu.VMEM, dtype=jnp.bfloat16)
    piece = (48, 128)
    return [
        pltpu.VMEM((2, 2, RING) + gate_block, jnp.bfloat16),
        pltpu.VMEM((2, RING) + down_block, jnp.bfloat16),
        pltpu.VMEM((2, RING, RING, nz) + piece, jnp.bfloat16),
        pltpu.VMEM((chunks, 2, RING // 2, nz) + piece, jnp.bfloat16),
        pltpu.VMEM((chunks, 2, RING, nz) + piece, jnp.bfloat16),
        pltpu.VMEM((chunks, RING, nz) + piece, jnp.bfloat16),
        pltpu.VMEM((chunks, 2, nz // 2) + piece, jnp.bfloat16),
        pltpu.VMEM((chunks, 2, nz) + piece, jnp.bfloat16),
        pltpu.VMEM((chunks, nz) + piece, jnp.bfloat16),
        pltpu.VMEM((chunks, nz) + piece, jnp.bfloat16),
        pltpu.VMEM((chunks, RING, nz) + piece, jnp.bfloat16),
        pltpu.SemaphoreType.DMA((2, chunks, 3)),
        pltpu.SemaphoreType.DMA((2, chunks, 6, 2)),
        pltpu.SemaphoreType.DMA((2, chunks, 2, nz)),
    ]


class Reduce:
    def __init__(self, p, bufs, own, gate_block, down_block, finish):
        self.p, self.own, self.finish = p, own, finish
        for name, ref in zip(SCRATCH, bufs, strict=True):
            setattr(self, name, ref)
        self.down_rows = down_block[0]
        self.gate, self.down = pieces(*gate_block, False), pieces(*down_block, True)
        self.stages = [self.s0, self.s1, self.s2, self.s3, self.s4, self.s5, self.s6, self.s7, self.s8, self.s9]

    def peers(self):
        p = self.p
        return [p.partner, p.right, p.left, p.above, p.below] + [p.to_z(d) for d in range(1, p.nz)]

    def link(self, h, k, way, src, dst, device):
        return send(src, dst, (self.sem_l.at[0, h, k, way], self.sem_l.at[1, h, k, way]), device)

    def d2d(self, h, core):
        own = self.own(h)
        dst = [self.dg.at[h % 2, 0], self.dg.at[h % 2, 1], self.dd.at[h % 2]]
        return [
            send(own[i](core), dst[i], (self.sem_d.at[0, h, i], self.sem_d.at[1, h, i]), self.p.partner) for i in range(3)
        ]

    def s0(self, h):
        for one in self.d2d(h, 1 - self.p.core):
            one.start()

    def xs1(self, h):
        p = self.p
        block = self.part.at[h % 2, p.x_far]
        return [
            self.link(h, 0, 0, block.at[pl.ds(0, 2)], self.x1.at[h, 0], p.right),
            self.link(h, 0, 1, block.at[pl.ds(2, 2)], self.x1.at[h, 1], p.left),
        ]

    def xs2(self, h):
        p = self.p
        return [
            self.link(h, 1, 0, self.part.at[h % 2, p.x_right], self.x2.at[h, 0], p.right),
            self.link(h, 1, 1, self.part.at[h % 2, p.x_left], self.x2.at[h, 1], p.left),
        ]

    def ys1(self, h):
        p = self.p
        block, half = self.yb.at[h, p.y_far], p.nz // 2
        return [
            self.link(h, 2, 0, block.at[pl.ds(0, half)], self.y1.at[h, 0], p.above),
            self.link(h, 2, 1, block.at[pl.ds(half, half)], self.y1.at[h, 1], p.below),
        ]

    def ys2(self, h):
        p = self.p
        return [
            self.link(h, 3, 0, self.yb.at[h, p.y_above], self.y2.at[h, 0], p.above),
            self.link(h, 3, 1, self.yb.at[h, p.y_below], self.y2.at[h, 1], p.below),
        ]

    def zs(self, h, d):
        p = self.p
        to = p.at_z(d)
        return send(self.zb.at[h, to], self.zr.at[h, p.z], (self.sem_z.at[0, h, 0, to], self.sem_z.at[1, h, 0, p.z]), p.to_z(d))

    def zs_from(self, h, d):
        p = self.p
        src = p.at_z(d)
        return send(self.zb.at[h, src], self.zr.at[h, src], (self.sem_z.at[0, h, 0, src], self.sem_z.at[1, h, 0, src]), p.to_z(d))

    def za(self, h, d):
        p = self.p
        mine = self.out.at[h, p.y, p.z]
        return send(mine, mine, (self.sem_z.at[0, h, 1, p.at_z(d)], self.sem_z.at[1, h, 1, p.z]), p.to_z(d))

    def za_from(self, h, d):
        p = self.p
        src = p.at_z(d)
        piece = self.out.at[h, p.y, src]
        return send(piece, piece, (self.sem_z.at[0, h, 1, src], self.sem_z.at[1, h, 1, src]), p.to_z(d))

    def ya1(self, h, y=None):
        p = self.p
        piece = self.out.at[h, p.y]
        return [self.link(h, 4, 0, piece, piece, p.above), self.link(h, 4, 1, piece, piece, p.below)]

    def ya1_from(self, h):
        p = self.p
        below, above = self.out.at[h, p.y_below], self.out.at[h, p.y_above]
        return [self.link(h, 4, 0, below, below, p.above), self.link(h, 4, 1, above, above, p.below)]

    def ya2(self, h, first, second):
        p, half = self.p, self.p.nz // 2
        a, b = self.out.at[h, first, pl.ds(0, half)], self.out.at[h, second, pl.ds(half, half)]
        return [self.link(h, 5, 0, a, a, p.above), self.link(h, 5, 1, b, b, p.below)]

    def s1(self, h):
        p = self.p
        for one in self.d2d(h, 1 - p.core):
            one.wait_recv()
            one.wait_send()
        own = self.own(h)

        def block(x, _):
            for i, cut in ((0, self.gate), (1, self.gate), (2, self.down)):
                mine = own[i](p.core).at[x]
                theirs = self.dd.at[h % 2, x] if i == 2 else self.dg.at[h % 2, i, x]
                for q in range(RING):
                    for k, (rows, columns) in enumerate(cut[q]):
                        total = wide(mine[rows, columns]) + wide(theirs[rows, columns])
                        self.part[h % 2, x, q, k, 16 * i : 16 * i + 16, :] = total.astype(jnp.bfloat16)

        loop(RING, block)
        for one in self.xs1(h):
            one.start()

    def s2(self, h):
        p = self.p
        for way, one in enumerate(self.xs1(h)):
            one.wait_recv()
        for way in WAYS:
            to = (p.x_right, p.x_left)[way]

            def add(k, _):
                q, kk = 2 * way + k // p.nz, k % p.nz
                total = wide(self.part[h % 2, to, q, kk]) + wide(self.x1[h, way, k // p.nz, kk])
                self.part[h % 2, to, q, kk] = total.astype(jnp.bfloat16)

            loop(2 * p.nz, add)
            self.xs2(h)[way].start()

    def s3(self, h):
        p = self.p
        for one in self.xs2(h):
            one.wait_recv()
        for one in self.xs1(h) + self.xs2(h):
            one.wait_send()

        def add(k, _):
            q, kk = k // p.nz, k % p.nz
            total = wide(self.part[h % 2, p.x, q, kk]) + (wide(self.x2[h, 0, q, kk]) + wide(self.x2[h, 1, q, kk]))
            self.yb[h, q, kk] = total.astype(jnp.bfloat16)

        loop(RING * p.nz, add)
        for one in self.ys1(h):
            one.start()

    def s4(self, h):
        p, half = self.p, self.p.nz // 2
        for one in self.ys1(h):
            one.wait_recv()
        for way in WAYS:
            to = (p.y_above, p.y_below)[way]
            for k in range(half):
                kk = way * half + k
                self.yb[h, to, kk] = (wide(self.yb[h, to, kk]) + wide(self.y1[h, way, k])).astype(jnp.bfloat16)
            self.ys2(h)[way].start()

    def s5(self, h):
        p = self.p
        for one in self.ys2(h):
            one.wait_recv()
        for k in range(p.nz):
            total = wide(self.yb[h, p.y, k]) + (wide(self.y2[h, 0, k]) + wide(self.y2[h, 1, k]))
            self.zb[h, k] = total.astype(jnp.bfloat16)
        for d in range(1, p.nz):
            self.zs(h, d).start()

    def s6(self, h):
        p = self.p
        total = wide(self.zb[h, p.z])
        for d in range(1, p.nz):
            self.zs_from(h, d).wait_recv()
            total += wide(self.zr[h, p.at_z(d)])
        self.out[h, p.y, p.z] = total.astype(jnp.bfloat16)
        for d in range(1, p.nz):
            self.za(h, d).start()

    def s7(self, h):
        for d in range(1, self.p.nz):
            self.za_from(h, d).wait_recv()
        for one in self.ya1(h):
            one.start()

    def s8(self, h):
        p = self.p
        for one in self.ya1_from(h):
            one.wait_recv()
        for one in self.ya2(h, p.y_below, p.y_above):
            one.start()

    def s9(self, h):
        p = self.p
        for one in self.ya2(h, p.y_far, p.y_far):
            one.wait_recv()
        self.finish(h)

    def drain(self, h):
        p = self.p
        for one in self.ys1(h) + self.ys2(h):
            one.wait_send()
        for d in range(1, p.nz):
            self.zs(h, d).wait_send()
            self.za(h, d).wait_send()
        for one in self.ya1(h) + self.ya2(h, p.y_below, p.y_above):
            one.wait_send()

    def unpack(self, h, b, unit, outs):
        for q in range(RING):
            for k, (rows, columns) in enumerate(self.gate[q]):
                for i in (0, 1):
                    for c in range(columns.start, columns.stop, unit):
                        to = pl.ds(pl.multiple_of(2 * c + b * unit, min(unit, 128)), min(unit, 128))
                        part = slice(c - columns.start, c - columns.start + unit)
                        outs[i][rows, to] = self.out[h, q, k, 16 * i : 16 * i + 16, part]
            for k, (rows, columns) in enumerate(self.down[q]):
                to = pl.ds(pl.multiple_of(b * self.down_rows + rows.start, 16), 16)
                outs[2][to, columns] = self.out[h, q, k, 32:48, :]


class Spread:
    def __init__(self, p, ins, outs, snd, rcv, loc):
        self.p, self.ins, self.outs, self.snd, self.rcv, self.loc = p, ins, outs, snd, rcv, loc

    def block(self, l, i, x, y=None, half=None):
        ref = self.outs[i].at[l, 2 * x + self.p.core]
        return ref if y is None else self.part(ref, y, half)

    def part(self, ref, y, half=None):
        rows, columns = ref.shape[0] // RING, ref.shape[1] // 2
        some = pl.ds(pl.multiple_of(y * rows, rows), rows)
        return ref.at[some] if half is None else ref.at[some, pl.ds(half * columns, columns)]

    def copy(self, l, i, k, src, dst, device):
        n = 2 * l + i - 1
        return send(src, dst, (self.snd.at[n, k], self.rcv.at[n, k]), device)

    def local(self, l, i):
        return pltpu.make_async_copy(self.ins[i].at[l], self.block(l, i, self.p.x), self.loc.at[3 * l + i])

    def own(self, l, i):
        return self.copy(l, i, 0, self.ins[i].at[l], self.block(l, i, self.p.x), self.p.partner)

    def x1(self, l, i, way):
        p = self.p
        src = self.part(self.ins[i].at[l], p.y)
        return self.copy(l, i, 1 + way, src, self.block(l, i, p.x, p.y), (p.right, p.left)[way])

    def x2(self, l, i, way):
        p = self.p
        b = self.block(l, i, (p.x_left, p.x_right)[way], p.y, way)
        return self.copy(l, i, 3 + way, b, b, (p.right, p.left)[way])

    def y1(self, l, i, n, way):
        p = self.p
        b = self.block(l, i, p.at_x(n + 1), p.y)
        return self.copy(l, i, 5 + 2 * n + way, b, b, (p.above, p.below)[way])

    def y2(self, l, i, n, way):
        p = self.p
        b = self.block(l, i, p.at_x(n + 1), (p.y_below, p.y_above)[way], way)
        return self.copy(l, i, 11 + 2 * n + way, b, b, (p.above, p.below)[way])

    def over(self, l, i, n):
        b = self.block(l, i, self.p.at_x(n + 1))
        return self.copy(l, i, 17 + n, b, b, self.p.partner)

    def f1(self, l, i):
        for way in WAYS:
            self.x1(l, i, way).start()
        self.local(l, i).start()
        self.own(l, i).start()

    def f2(self, l, i):
        for way in WAYS:
            self.x1(l, i, way).wait_recv()
            self.x2(l, i, way).start()
            for to in (0, 1):
                self.y1(l, i, (2, 0)[way], to).start()

    def f3(self, l, i):
        for way in WAYS:
            self.x2(l, i, way).wait_recv()
        for to in (0, 1):
            self.y1(l, i, 1, to).start()

    def f4(self, l, i):
        def go(n, _):
            for way in WAYS:
                self.y1(l, i, (n + 2) % 3, way).wait_recv()
                self.y2(l, i, (n + 2) % 3, way).start()

        loop(3, go)

    def f5(self, l, i):
        def go(n, _):
            for way in WAYS:
                self.y2(l, i, (n + 2) % 3, way).wait_recv()
            self.over(l, i, (n + 2) % 3).start()

        loop(3, go)

    def f6(self, l, i):
        self.local(l, i).wait()
        self.own(l, i).wait_recv()

        def go(n, _):
            self.over(l, i, n).wait_recv()

        loop(3, go)

    def drain(self, l, i):
        self.own(l, i).wait_send()
        for way in WAYS:
            self.x1(l, i, way).wait_send()
            self.x2(l, i, way).wait_send()

        def go(n, _):
            for way in WAYS:
                self.y1(l, i, n, way).wait_send()
                self.y2(l, i, n, way).wait_send()
            self.over(l, i, n).wait_send()

        loop(3, go)


def nt(a, b):
    return lax.dot_general(a, b, (((1,), (1,)), ((), ())), preferred_element_type=jnp.float32)


def nn(a, b):
    return jnp.dot(a, b, preferred_element_type=jnp.float32)


def scaled(h):
    w = wide(h)
    return w, lax.rsqrt(jnp.mean(w * w, -1, keepdims=True) + 1e-6)


class Compute:
    def __init__(self, bufs, block):
        (self.wg, self.wu, self.wd, self.h, self.dy, self.dyt, self.a, self.at, self.acc, self.act, self.dg, self.du, self.sums) = bufs
        self.block = block
        self.tokens, self.d = self.h.shape
        self.unit = self.wg.shape[3] // 16

    def each(self, body):
        def go(i, _):
            body(i, pl.ds(pl.multiple_of(i * self.block, self.block), self.block))

        loop(self.tokens // self.block, go)

    def enter(self, rows):
        w, scale = scaled(self.h[rows, :])
        self.a[0, rows, :] = (w * scale).astype(jnp.bfloat16)

    def turn_dy(self, rows):
        self.dyt[:, rows] = self.dy[rows, :].T

    def turn_a(self, l, rows):
        self.at[:, rows] = self.a[l, rows, :].T

    def forward(self, rows):
        a = self.a[0, rows, :]
        total = jnp.zeros((self.block, self.d), jnp.float32)
        ff = 16 * self.unit
        for j in range(4):
            cut = slice(j * ff // 4, (j + 1) * ff // 4)
            gate = nn(a, self.wg[0, :, :, cut].reshape(self.d, -1))
            up = nn(a, self.wu[0, :, :, cut].reshape(self.d, -1))
            act = (gate * lax.logistic(gate) * up).astype(jnp.bfloat16)
            total += nn(act, self.wd[0, 2 * j : 2 * j + 2].reshape(-1, self.d))
        h = self.h[rows, :] + total.astype(jnp.bfloat16)
        self.h[rows, :] = h
        w, scale = scaled(h)
        a = (w * scale).astype(jnp.bfloat16)
        self.a[1, rows, :] = a
        self.at[:, rows] = a.T

    def tile(self, l, n, last=None):
        u = self.unit
        b, x, slot = n // 4, n % 4, n % 2
        cuts = [pl.ds(pl.multiple_of((2 * x + c) * 2 * u + b * u, min(u, 128)), u) for c in (0, 1)]
        wg, wu = (
            jnp.concatenate([w[l, :, :, cut].reshape(self.d, u) for cut in cuts], axis=1) for w in (self.wg, self.wu)
        )
        wd = self.wd[l, pl.ds(2 * x, 2), pl.ds(pl.multiple_of(b * u, min(u, 128)), u), :].reshape(2 * u, self.d)

        def tokens(i, rows):
            a, dy = self.a[l, rows, :], self.dy[rows, :]
            gate, up, dact = nn(a, wg), nn(a, wu), nt(dy, wd)
            if last is not None:
                self.weigh(rows, 1 - slot)
            dact = wide(dact.astype(jnp.bfloat16))
            sig = lax.logistic(gate)
            silu = gate * sig
            dg = (dact * up * (sig + silu * (1 - sig))).astype(jnp.bfloat16)
            du = (dact * silu).astype(jnp.bfloat16)
            self.act[slot, rows, :] = (silu * up).astype(jnp.bfloat16)
            self.dg[slot, rows, :] = dg
            self.du[slot, rows, :] = du
            if l == 1:
                self.acc[rows, :] += nt(dg, wg) + nt(du, wu)

        self.each(tokens)
        if last is not None:
            self.settle((n - 1) % 4, *last)

    def weigh(self, rows, slot):
        for j, (left, right) in enumerate(((self.at, self.dg), (self.at, self.du), (self.dyt, self.act))):
            self.sums[j] += nn(left[:, rows], right[slot, rows, :])

    def settle(self, x, gate_to, up_to, down_to):
        u = self.unit
        columns = pl.ds(pl.multiple_of(2 * x * u, min(2 * u, 128)), 2 * u)
        for j, to in enumerate((gate_to, up_to)):
            to[:, :, :, columns] = self.sums[j].astype(jnp.bfloat16).reshape(RING, 2, self.d // 8, 2 * u)
        down_to[x] = self.sums[2].T.astype(jnp.bfloat16).reshape(2, u, self.d)
        self.sums[...] = jnp.zeros_like(self.sums)

    def back(self, rows):
        w, scale = scaled(self.h[rows, :])
        da = wide(self.acc[rows, :].astype(jnp.bfloat16))
        dot = jnp.sum(da * w, -1, keepdims=True) * (1.0 / self.d)
        dh = da * scale - w * (scale * scale * scale * dot)
        dy = self.dy[rows, :] + dh.astype(jnp.bfloat16)
        self.dy[rows, :] = dy
        self.dyt[:, rows] = dy.T
        self.at[:, rows] = self.a[0, rows, :].T


AFTER = (0, 1, 2, 5, 6, 8, 10, 12, 14, 15)


def step_kernel(nz, block, gate_block, down_block, *refs):
    x_in, dy_in, *rest = refs
    shards, outs, rest = rest[:3], rest[3:6], rest[6:]
    bufs, (own_g, own_d), reds, (snd, rcv, loc, io, snd_y, rcv_y) = rest[:13], rest[13:15], rest[15:29], rest[29:]
    p = Place(nz)
    comp = Compute(bufs, block)
    unit, chunks = comp.unit, 4

    def own(h):
        return (
            lambda core: own_g.at[h % 2, 0, :, core],
            lambda core: own_g.at[h % 2, 1, :, core],
            lambda core: own_d.at[h % 2, :, core],
        )

    def finish(h):
        l, b = 1 - h // 2, h % 2
        red.unpack(h, b, unit, [o.at[l] for o in outs])

    red = Reduce(p, reds, own, gate_block, down_block, finish)
    gat = Gather(p, shards, bufs[:3], snd, rcv, loc)
    spr = Spread(p, shards, bufs[:3], snd_y, rcv_y, loc)
    into = [pltpu.make_async_copy(x_in, comp.h, io.at[0]), pltpu.make_async_copy(dy_in, comp.dy, io.at[1])]
    for one in into:
        one.start()
    meet(red.peers())
    for i in SPREAD:
        spr.f1(0, i)
    into[0].wait()
    for i in SPREAD:
        spr.f2(0, i)
    gat.first(0, 0)
    comp.each(lambda i, rows: comp.enter(rows))
    for i in SPREAD:
        spr.f3(0, i)
    into[1].wait()
    comp.each(lambda i, rows: comp.turn_dy(rows))
    comp.acc[...] = jnp.zeros_like(comp.acc)
    comp.sums[...] = jnp.zeros_like(comp.sums)
    gat.second(0, 0)
    for i in SPREAD:
        spr.f4(0, i)
        spr.f1(1, i)
    gat.third(0, 0)
    for i in SPREAD:
        spr.f2(1, i)
    gat.first(1, 0)
    for i in SPREAD:
        spr.f5(0, i)
    gat.last(0, 0)
    for i in SPREAD:
        spr.f6(0, i)
    for i in SPREAD:
        spr.f3(1, i)

    def ahead(i, rows):
        comp.forward(rows)

        @pl.when(i == 0)
        def _():
            gat.second(1, 0)
            spr.f4(1, 1)

        @pl.when(i == 1)
        def _():
            spr.f4(1, 2)
            gat.third(1, 0)

        pl.when(i == 2)(lambda: spr.f5(1, 1))

    comp.each(ahead)
    spr.f5(1, 2)
    gat.last(1, 0)
    for i in SPREAD:
        spr.f6(1, i)

    def tick(t):
        for k, (stage, after) in enumerate(zip(red.stages, AFTER, strict=True)):
            since = t - 4 - after
            h = 2 * (since // 8) + (since % 8) // 3
            due = (since >= 0) & (since < 16) & ((since % 8 == 0) | (since % 8 == 3))
            pl.when(due)(lambda stage=stage, h=h: stage(h))

    def terms(n):
        slot = n // 4 % 2
        return own_g.at[slot, 0], own_g.at[slot, 1], own_d.at[slot]

    for l in (1, 0):
        base = 8 * (1 - l)
        comp.tile(l, 0)

        def tile(n, _):
            tick(base + n - 1)
            comp.tile(l, n, terms(n - 1))

        loop(8, tile, 1)
        comp.each(lambda i, rows: comp.weigh(rows, 1))
        comp.settle(3, *terms(7))
        tick(base + 7)
        if l == 1:
            comp.each(lambda i, rows: comp.back(rows))

    def late(t, _):
        tick(t)

    loop(16 + AFTER[-1], late, 16)

    def drain(h, _):
        red.drain(h)

    loop(chunks, drain)
    def rest(l, _):
        gat.drain(l, 0)
        for i in SPREAD:
            spr.drain(l, i)

    loop(2, rest)


def compute_scratch(tokens, d, ff):
    unit = ff // 16
    bf = jnp.bfloat16
    return [
        pltpu.VMEM((2, 8, d // 8, ff), bf),
        pltpu.VMEM((2, 8, d // 8, ff), bf),
        pltpu.VMEM((2, 8, ff // 8, d), bf),
        pltpu.VMEM((tokens, d), bf),
        pltpu.VMEM((tokens, d), bf),
        pltpu.VMEM((d, tokens), bf),
        pltpu.VMEM((2, tokens, d), bf),
        pltpu.VMEM((d, tokens), bf),
        pltpu.VMEM((tokens, d), jnp.float32),
        pltpu.VMEM((2, tokens, 2 * unit), bf),
        pltpu.VMEM((2, tokens, 2 * unit), bf),
        pltpu.VMEM((2, tokens, 2 * unit), bf),
        pltpu.VMEM((3, d, 2 * unit), jnp.float32),
    ]


def gradients_of(mesh, x, dy, weights):
    nz = mesh.shape["r"] // RING
    tokens, d = x.shape
    ff = weights[0].shape[2]
    gate_block, down_block = (d // 8, ff // 2), (ff // 16, d)
    any_space, vmem = pl.BlockSpec(memory_space=pl.ANY), pl.BlockSpec(memory_space=pltpu.VMEM)
    return pl.pallas_call(
        functools.partial(step_kernel, nz, min(512, tokens // 4), gate_block, down_block),
        out_shape=[jax.ShapeDtypeStruct(w.shape, w.dtype) for w in weights],
        in_specs=[any_space] * 5,
        out_specs=[vmem] * 3,
        scratch_shapes=compute_scratch(tokens, d, ff)
        + [
            pltpu.VMEM((2, 2, RING, 2) + gate_block, jnp.bfloat16),
            pltpu.VMEM((2, RING, 2) + down_block, jnp.bfloat16),
        ]
        + reduce_scratch(nz, 4, gate_block, down_block)
        + [
            pltpu.SemaphoreType.DMA((6, 9)),
            pltpu.SemaphoreType.DMA((6, 9)),
            pltpu.SemaphoreType.DMA((6,)),
            pltpu.SemaphoreType.DMA((2,)),
            pltpu.SemaphoreType.DMA((4, 20)),
            pltpu.SemaphoreType.DMA((4, 20)),
        ],
        compiler_params=pltpu.CompilerParams(collective_id=0, has_side_effects=True, vmem_limit_bytes=67043328),
        name="step",
    )(x, dy, *weights)


def solution(mesh):
    def step(x, dy, *arrays):
        weights, m, v = (arrays[i : i + 3] for i in (0, 3, 6))
        gradients = [g.astype(jnp.float32) for g in gradients_of(mesh, x[0], dy[0], weights)]
        new = [adamw(w.astype(jnp.float32), m, v, g) for w, m, v, g in zip(weights, m, v, gradients, strict=True)]
        return tuple(one[which] for which in range(3) for one in new)

    states, cut = P(("rep", "r", "s"), None, None), P(None, "s", None)
    return jax.shard_map(
        step,
        mesh=mesh,
        in_specs=(states, states) + (cut,) * 9,
        out_specs=(P("rep", "s", None),) * 9,
        check_vma=False,
    )
```
